512 devices in a mesh: dp: 8 (over y, core), seq: 16 (over z), head: 4 (over x).
Axes of the slice: x: 4, y: 4, z: 16, core: 2. Of those that a mesh axis runs over, the one named last changes fastest.
Arguments:
- queries: bfloat16 [8, 4096, 3072], P('dp', 'seq', 'head'), may hold values from -60 to 60
- key_rows: bfloat16 [8, 4096, 3072], P('dp', 'seq', 'head'), may hold values from -4.5 to 4.5
- value_rows: bfloat16 [8, 4096, 3072], P('dp', 'seq', 'head'), may hold values from -4 to 4
- out_grad: bfloat16 [8, 4096, 3072], P('dp', 'seq', 'head'), may hold values from -9.5 to 9.5
- tile_image: int32 [8, 32], P('dp'), may hold values from 0 to 7, never falling along the last dimension, each value on 1 to 6 neighbouring positions
Outputs:
- attn_out: bfloat16 [8, 4096, 3072], P('dp', 'seq', 'head')
- query_grad: bfloat16 [8, 4096, 3072], P('dp', 'seq', 'head')
- key_grad: bfloat16 [8, 4096, 3072], P('dp', 'seq', 'head')
- value_grad: bfloat16 [8, 4096, 3072], P('dp', 'seq', 'head')
- grad_rms: float32 [], replicated
The draws below stay inside these ranges and needn't reach their ends.
Inputs may be any that keep to these rules, and one draw needn't show every extreme that they name: `tile_image`: image numbers never fall along a sequence; every image covers 1 to 6 whole tiles of 128 patches, and in each sequence one image covers exactly 6 tiles.
All inputs are finite; a program needn't handle non-finite values.
Results may differ from the reference program's by a relative error of at most 0.0073.
Values may be sent and summed in bfloat16 or wider, within the bound.
A program may use at most 64 MiB of HBM per device.

```python
import math
import jax
import jax.numpy as jnp
import numpy as np
from jax import lax

HEAD_DIM = 128
HEADS = 24
TILE = 128
MOST = 6
LEN = 4096
TILES = 32
IMAGES = 8
SEQS = 8


def paired(key):
    array_shape = (SEQS, LEN, HEADS * HEAD_DIM)
    base_key = jax.random.fold_in(key, 7001)
    query_key, key_key = jax.random.split(base_key, 2)
    query_draw = jax.random.truncated_normal(query_key, -4.0, 4.0, array_shape, jnp.float32)
    key_draw = jax.random.truncated_normal(key_key, -4.0, 4.0, array_shape, jnp.float32)
    return (query_draw, key_draw)


def draw_queries(key, part):
    return paired(key)[0].astype(jnp.bfloat16)


def draw_key_rows(key, part):
    return paired(key)[1].astype(jnp.bfloat16)


def draw_out_grad(key, part):
    array_shape = (SEQS, LEN, HEADS * HEAD_DIM)
    base_key = jax.random.fold_in(key, 7003)
    noise = jax.random.truncated_normal(base_key, -4.0, 4.0, array_shape, jnp.float32)
    seq_ramp = jnp.arange(SEQS, dtype=jnp.float32)[:, None, None] / max(SEQS - 1, 1)
    place_ramp = jnp.arange(LEN, dtype=jnp.float32)[None, :, None] / (LEN - 1)
    feature_ramp = jnp.arange(HEADS * HEAD_DIM, dtype=jnp.float32)[None, None, :] / (HEADS * HEAD_DIM - 1)
    factor = 3.0 ** (0.5 * (seq_ramp + place_ramp + feature_ramp) - 0.75)
    return (noise * factor).astype(jnp.bfloat16)


def block_levels(stream_key, shape, pieces, low, top_value):
    gain, own = 1.0, jax.random.fold_in(stream_key, 6)
    for dim, blocks in pieces:
        draws = jnp.exp(jax.random.uniform(jax.random.fold_in(own, dim), (blocks,), jnp.float32, low / len(pieces), top_value / len(pieces)))
        gain = gain * jnp.repeat(draws, shape[dim] // blocks).reshape([-1 if axis == dim else 1 for axis in range(len(shape))])
    return gain


def profile(count, total, most, skew):
    portions = [(1 << 20) // math.isqrt(grade ** skew) + 1 for grade in range(2, count + 1)]
    rest, holding = total - most - (count - 1), [1] * (count - 1)
    while rest > 0:
        movable = [i for i in range(count - 1) if holding[i] < most]
        pool, remaining = sum([portions[i] for i in movable]), rest
        for i in movable:
            more = min(most - holding[i], max(1, remaining * portions[i] // pool), rest)
            holding[i] = holding[i] + more
            rest = rest - more
    return np.array([most] + holding)


def uneven_parts(own_key, number_of, total, reach, skew):
    if number_of == 2:
        one = jax.random.randint(own_key, (), max(1, total - reach), min(reach, total - 1) + 1)
        return jnp.stack([one, total - one])
    sizes = jnp.asarray(profile(number_of, total, reach, skew), jnp.int32)
    pairs = (number_of - 1) // 2
    giver, sink = sizes[1:1 + 2 * pairs:2], sizes[2:2 + 2 * pairs:2]
    slack = jnp.minimum(giver - 1, reach - sink)
    shifted = jax.random.randint(jax.random.fold_in(own_key, 1), (pairs,), 0, 1 << 20) % (slack + 1)
    sizes = sizes.at[1:1 + 2 * pairs:2].set(giver - shifted).at[2:2 + 2 * pairs:2].set(sink + shifted)
    return sizes[jax.random.permutation(jax.random.fold_in(own_key, 2), number_of)]


def centred(own_key, shape, spread, reach, cuts=(), held_as=jnp.bfloat16):
    drawn = spread * jax.random.normal(own_key, shape, jnp.float32)
    if cuts:
        drawn = drawn * block_levels(own_key, shape, cuts, -0.22, 0.18)
    return jnp.clip(drawn, -reach, reach).astype(held_as)


def setup_inputs(seed: int = 0) -> dict:
    seeds = jax.random.split(jax.random.key(seed), 6)
    return {
        "queries": draw_queries(jax.random.fold_in(seeds[5], 71), 0),
        "key_rows": draw_key_rows(jax.random.fold_in(seeds[5], 71), 0),
        "value_rows": centred(seeds[2], (SEQS, LEN, HEADS * HEAD_DIM), 1.0, 4.0, ((0, 8), (1, 16), (2, 4))),
        "out_grad": draw_out_grad(jax.random.fold_in(seeds[5], 71), 0),
        "tile_image": jax.vmap(lambda own: jnp.searchsorted(jnp.cumsum(uneven_parts(own, IMAGES, TILES, MOST, 2)), jnp.arange(TILES), side="right"))(jax.random.split(seeds[4], SEQS)).reshape((SEQS, TILES)).astype(jnp.int32),
    }


def product(first_operand, second_operand):
    return jnp.dot(first_operand, second_operand, precision=lax.Precision.HIGHEST, preferred_element_type=jnp.float32)

def attend_head(query_head, key_head, value_head, grad_head, token_image):
    scale_value = HEAD_DIM ** (-0.5)
    query_wide = query_head.astype(jnp.float32)
    key_wide = key_head.astype(jnp.float32)
    value_wide = value_head.astype(jnp.float32)
    grad_wide = grad_head.astype(jnp.float32)
    same_image = token_image[:, None] == token_image[None, :]
    scores = jnp.where(same_image, product(query_wide, key_wide.T) * scale_value, -jnp.inf)
    row_max = lax.optimization_barrier(jnp.max(scores, axis=1, keepdims=True))
    log_sum = row_max + jnp.log(lax.optimization_barrier(jnp.sum(jnp.exp(scores - row_max), axis=1, keepdims=True)))
    weights = jnp.exp(scores - log_sum).astype(jnp.bfloat16)
    weights_wide = lax.optimization_barrier(weights).astype(jnp.float32)
    attended = product(weights_wide, value_wide).astype(jnp.bfloat16)
    attended_wide = lax.optimization_barrier(attended).astype(jnp.float32)
    row_delta = lax.optimization_barrier(jnp.sum(grad_wide * attended_wide, axis=1, keepdims=True))
    dweights = product(grad_wide, value_wide.T)
    dscores = (weights_wide * (dweights - row_delta) * scale_value).astype(jnp.bfloat16)
    dscores_wide = lax.optimization_barrier(dscores).astype(jnp.float32)
    query_grad = product(dscores_wide, key_wide).astype(jnp.bfloat16)
    key_grad = product(dscores_wide.T, query_wide).astype(jnp.bfloat16)
    value_grad = product(weights_wide.T, grad_wide).astype(jnp.bfloat16)
    return (attended, query_grad, key_grad, value_grad)

def to_heads(array):
    return array.reshape(LEN, HEADS, HEAD_DIM).transpose(1, 0, 2)

def from_heads(array):
    return array.transpose(1, 0, 2).reshape(LEN, HEADS * HEAD_DIM)

def reference(queries, key_rows, value_rows, out_grad, tile_image):

    def one_sequence(sequence_item):
        query_seq, key_seq, value_seq, grad_seq, tile_row = sequence_item
        token_image = jnp.repeat(tile_row.astype(jnp.int32), TILE, total_repeat_length=LEN)

        def one_head(head_item):
            return attend_head(head_item[0], head_item[1], head_item[2], head_item[3], token_image)
        results = lax.map(one_head, (to_heads(query_seq), to_heads(key_seq), to_heads(value_seq), to_heads(grad_seq)))
        return tuple((from_heads(member) for member in results))
    attended, query_grad, key_grad, value_grad = lax.map(one_sequence, (queries, key_rows, value_rows, out_grad, tile_image))
    squares = jnp.sum(jnp.square(query_grad.astype(jnp.float32)))
    squares = squares + jnp.sum(jnp.square(key_grad.astype(jnp.float32)))
    squares = squares + jnp.sum(jnp.square(value_grad.astype(jnp.float32)))
    grad_rms = jnp.sqrt(squares / (3.0 * attended.size))
    return (attended, query_grad, key_grad, value_grad, grad_rms)
```

```python
import functools

import jax
import jax.numpy as jnp
from jax import lax
from jax.experimental import pallas as pl
from jax.experimental.pallas import tpu as pltpu
from jax.sharding import PartitionSpec as P

HEAD_DIM = 128
TILE = 128
OWN = 2
WINDOW = 8
ROWS = WINDOW * TILE
BLOCK = 256
MESH = pl.DeviceIdType.MESH


def rows_of(tile, count=1):
    return pl.ds(tile * TILE, count * TILE)


def kernel(
    tiles_ref,
    q_hbm,
    k_hbm,
    v_hbm,
    g_hbm,
    o_ref,
    dq_ref,
    dk_ref,
    dv_ref,
    rms_ref,
    win,
    outs,
    stage,
    got_a,
    got_b,
    bias,
    dk_acc,
    dv_acc,
    squares,
    line_sums,
    plane_sums,
    load_sem,
    own_send,
    own_recv,
    a_send,
    a_recv,
    b_send,
    b_recv,
    line_send,
    line_recv,
    plane_send,
    plane_recv,
    *,
    heads,
    line,
    dps,
    heads_axis,
    total,
):
    me = lax.axis_index("seq")
    my_dp = lax.axis_index("dp")
    my_head = lax.axis_index("head")
    scale = HEAD_DIM ** (-0.5)
    has_left = me > 0
    has_right = me < line - 1
    left = jnp.maximum(me - 1, 0)
    right = jnp.minimum(me + 1, line - 1)
    tile_count = OWN * line

    def load(source, slot, head):
        return pltpu.make_async_copy(
            source.at[0, :, pl.ds(head * HEAD_DIM, HEAD_DIM)],
            win.at[head, slot, rows_of(3, 2), :],
            load_sem.at[head, slot],
        )

    def own_copy(head, way):
        return pltpu.make_async_remote_copy(
            src_ref=win.at[head, :, rows_of(3, 2), :],
            dst_ref=win.at[head, :, rows_of(1 if way == 0 else 5, 2), :],
            send_sem=own_send.at[way, head],
            recv_sem=own_recv.at[way, head],
            device_id={"seq": right if way == 0 else left},
            device_id_type=MESH,
        )

    def a_copy(head, way):
        return pltpu.make_async_remote_copy(
            src_ref=stage.at[way, head],
            dst_ref=got_a.at[way, head],
            send_sem=a_send.at[way, head],
            recv_sem=a_recv.at[way, head],
            device_id={"seq": right if way == 0 else left},
            device_id_type=MESH,
        )

    def b_copy(head, way):
        return pltpu.make_async_remote_copy(
            src_ref=outs.at[head, :, rows_of(6 if way == 0 else 1), :],
            dst_ref=got_b.at[way, head],
            send_sem=b_send.at[way, head],
            recv_sem=b_recv.at[way, head],
            device_id={"seq": right if way == 0 else left},
            device_id_type=MESH,
        )

    def each_start(copy, head):
        @pl.when(has_right)
        def _():
            copy(head, 0).start()

        @pl.when(has_left)
        def _():
            copy(head, 1).start()

    def each_wait_recv(copy, head):
        @pl.when(has_left)
        def _():
            copy(head, 0).wait_recv()

        @pl.when(has_right)
        def _():
            copy(head, 1).wait_recv()

    def each_wait_send(copy, head):
        @pl.when(has_right)
        def _():
            copy(head, 0).wait_send()

        @pl.when(has_left)
        def _():
            copy(head, 1).wait_send()

    for head in range(heads):
        for slot, source in enumerate((q_hbm, k_hbm, v_hbm, g_hbm)):
            load(source, slot, head).start()

    @pl.when(jnp.logical_not(has_left))
    def _():
        win[:, :, rows_of(0, 3), :] = jnp.zeros((heads, 4, 3 * TILE, HEAD_DIM), jnp.bfloat16)

    @pl.when(jnp.logical_not(has_right))
    def _():
        win[:, :, rows_of(5, 3), :] = jnp.zeros((heads, 4, 3 * TILE, HEAD_DIM), jnp.bfloat16)

    barrier = pltpu.get_barrier_semaphore()

    def greet_line(step, carry):
        pl.semaphore_signal(
            barrier,
            inc=1,
            device_id={"seq": lax.rem(me + step, line)},
            device_id_type=MESH,
        )
        return carry

    def plane_peer(step):
        place = lax.rem(my_dp * heads_axis + my_head + step, dps * heads_axis)
        return place // heads_axis, lax.rem(place, heads_axis)

    def greet_plane(step, carry):
        peer_dp, peer_head = plane_peer(step)
        pl.semaphore_signal(
            barrier,
            inc=1,
            device_id={"dp": peer_dp, "head": peer_head},
            device_id_type=MESH,
        )
        return carry

    lax.fori_loop(1, line, greet_line, 0)
    lax.fori_loop(1, dps * heads_axis, greet_plane, 0)

    images = []
    for place in range(WINDOW):
        tile = OWN * me - 3 + place
        image = tiles_ref[0, jnp.clip(tile, 0, tile_count - 1)]
        image = jnp.where(tile < 0, -1, image)
        images.append(jnp.where(tile >= tile_count, -2, image))
    over_left = images[0] == images[5]
    over_right = images[2] == images[7]
    names = list(images)
    names[0] = jnp.where(over_left, images[0], -3)
    names[7] = jnp.where(over_right, images[7], -4)
    for row in range(WINDOW):
        for column in range(WINDOW):
            level = jnp.where(names[row] == names[column], 0.0, -jnp.inf).astype(jnp.float32)
            bias[row : row + 1, column * TILE : (column + 1) * TILE] = jnp.full(
                (1, TILE), level, jnp.float32
            )
    not_left = jnp.logical_not(over_left)
    not_right = jnp.logical_not(over_right)
    from_left = [jnp.logical_and(images[w] == images[0], not_left) for w in (3, 4)]
    from_right = [jnp.logical_and(images[w] == images[7], not_right) for w in (3, 4)]
    mine = {}
    for w in (1, 2):
        mine[w] = jnp.logical_and(images[w] == images[5], not_left)
    for w in (5, 6):
        mine[w] = jnp.logical_and(images[w] == images[2], not_right)
    for index, w in enumerate((3, 4)):
        mine[w] = jnp.logical_not(jnp.logical_or(from_left[index], from_right[index]))
    squares[...] = jnp.zeros((8, 128), jnp.float32)

    pl.semaphore_wait(barrier, line - 1 + dps * heads_axis - 1)

    def send_own(head):
        for slot, source in enumerate((q_hbm, k_hbm, v_hbm, g_hbm)):
            load(source, slot, head).wait()
        each_start(own_copy, head)

    for head in range(min(2, heads)):
        send_own(head)

    def add_squares(value, flag):
        wide = value.astype(jnp.float32)
        wide = jnp.sum((wide * wide).reshape(TILE // 8, 8, HEAD_DIM), axis=0)
        squares[...] += jnp.where(flag, wide, 0.0)

    def compute(head):
        dk_acc[...] = jnp.zeros((HEAD_DIM, ROWS), jnp.float32)
        dv_acc[...] = jnp.zeros((HEAD_DIM, ROWS), jnp.float32)
        lanes = (((1,), (1,)), ((), ()))
        rows = (((0,), (0,)), ((), ()))
        wide = jnp.float32

        def block(index, carry):
            here = pl.ds(pl.multiple_of(index * BLOCK, BLOCK), BLOCK)
            query = win[head, 0, here, :]
            grad = win[head, 3, here, :]
            keys = win[head, 1]
            values = win[head, 2]
            scores = lax.dot_general(query, keys, lanes, preferred_element_type=wide) * scale
            pieces = []
            for half in range(BLOCK // TILE):
                row = bias[pl.ds(index * (BLOCK // TILE) + half, 1), :]
                pieces.append(scores[half * TILE : (half + 1) * TILE] + row)
            scores = jnp.concatenate(pieces, axis=0)
            raised = jnp.exp(scores - jnp.max(scores, axis=1, keepdims=True))
            weights = raised * (1.0 / jnp.sum(raised, axis=1, keepdims=True))
            weights = weights.astype(jnp.bfloat16)
            out = jnp.dot(weights, values, preferred_element_type=wide).astype(jnp.bfloat16)
            outs[head, 0, here, :] = out
            delta = jnp.sum(grad.astype(wide) * out.astype(wide), axis=1, keepdims=True)
            dweights = lax.dot_general(grad, values, lanes, preferred_element_type=wide)
            dscores = (weights.astype(wide) * (dweights - delta)).astype(jnp.bfloat16)
            dquery = jnp.dot(dscores, keys, preferred_element_type=wide) * scale
            outs[head, 1, here, :] = dquery.astype(jnp.bfloat16)
            dk_acc[...] += lax.dot_general(query, dscores, rows, preferred_element_type=wide)
            dv_acc[...] += lax.dot_general(grad, weights, rows, preferred_element_type=wide)
            return carry

        lax.fori_loop(0, ROWS // BLOCK, block, 0)
        for w in range(1, WINDOW - 1):
            dk = jnp.transpose(dk_acc[:, w * TILE : (w + 1) * TILE] * scale).astype(jnp.bfloat16)
            dv = jnp.transpose(dv_acc[:, w * TILE : (w + 1) * TILE]).astype(jnp.bfloat16)
            outs[head, 2, rows_of(w), :] = dk
            outs[head, 3, rows_of(w), :] = dv
            add_squares(outs[head, 1, rows_of(w), :], mine[w])
            add_squares(dk, mine[w])
            add_squares(dv, mine[w])

    out_refs = (o_ref, dq_ref, dk_ref, dv_ref)

    def assemble(head):
        column = pl.ds(pl.multiple_of(head * HEAD_DIM, HEAD_DIM), HEAD_DIM)
        each_wait_recv(b_copy, head)
        for slot, out_ref in enumerate(out_refs):
            first = outs[head, slot, rows_of(3), :]
            first = jnp.where(from_left[0], got_a[0, head + 1, slot], first)
            first = jnp.where(from_right[0], got_b[1, head, slot], first)
            out_ref[0, rows_of(0), column] = first
            second = outs[head, slot, rows_of(4), :]
            second = jnp.where(from_left[1], got_b[0, head, slot], second)
            second = jnp.where(from_right[1], got_a[1, head + 1, slot], second)
            out_ref[0, rows_of(1), column] = second

    def fill_stage(head, previous):
        for way, place, switch, back in ((0, 2, over_right, 5), (1, 5, over_left, 2)):
            for slot in range(4):
                passed = win[head, slot, rows_of(place), :]
                if previous is None:
                    other = jnp.zeros((TILE, HEAD_DIM), jnp.bfloat16)
                else:
                    other = outs[previous, slot, rows_of(back), :]
                stage[way, head, slot] = jnp.where(switch, passed, other)

    def step(head, carry):
        each_wait_recv(own_copy, head)

        @pl.when(head == 0)
        def _():
            fill_stage(head, None)

        @pl.when(head > 0)
        def _():
            fill_stage(head, head - 1)

        each_start(a_copy, head)

        @pl.when(head + 2 < heads)
        def _():
            send_own(head + 2)

        @pl.when(head > 0)
        def _():
            each_start(b_copy, head - 1)

        each_wait_recv(a_copy, head)
        blank = jnp.zeros((TILE, HEAD_DIM), jnp.bfloat16)
        for slot in range(4):
            win[head, slot, rows_of(0), :] = jnp.where(over_left, got_a[0, head, slot], blank)
            win[head, slot, rows_of(7), :] = jnp.where(over_right, got_a[1, head, slot], blank)
        compute(head)

        @pl.when(head >= 2)
        def _():
            assemble(head - 2)

        return carry

    lax.fori_loop(0, heads, step, 0)

    line_sums[pl.ds(me, 1)] = squares[...][None]

    def line_copy(step):
        return pltpu.make_async_remote_copy(
            src_ref=squares,
            dst_ref=line_sums.at[me],
            send_sem=line_send.at[step],
            recv_sem=line_recv.at[me],
            device_id={"seq": lax.rem(me + step, line)},
            device_id_type=MESH,
        )

    def line_arrival(step):
        peer = lax.rem(me + step, line)
        return pltpu.make_async_remote_copy(
            src_ref=squares,
            dst_ref=line_sums.at[peer],
            send_sem=line_send.at[step],
            recv_sem=line_recv.at[peer],
            device_id={"seq": peer},
            device_id_type=MESH,
        )

    def over(count, action):
        def body(step, carry):
            action(step)
            return carry

        lax.fori_loop(1, count, body, 0)

    over(line, lambda step: line_copy(step).start())

    fill_stage_last = ((0, 5), (1, 2))
    for way, back in fill_stage_last:
        for slot in range(4):
            stage[way, heads, slot] = outs[heads - 1, slot, rows_of(back), :]
    each_start(a_copy, heads)
    each_start(b_copy, heads - 1)

    if heads >= 2:
        assemble(heads - 2)

    over(line, lambda step: line_arrival(step).wait_recv())
    place = my_dp * heads_axis + my_head
    line_total = jnp.sum(line_sums[...], axis=0)
    squares_line = plane_sums.at[place]
    squares_line[...] = line_total

    def plane_copy(step, slot):
        peer_dp, peer_head = plane_peer(step)
        return pltpu.make_async_remote_copy(
            src_ref=plane_sums.at[place],
            dst_ref=plane_sums.at[slot],
            send_sem=plane_send.at[step],
            recv_sem=plane_recv.at[slot],
            device_id={"dp": peer_dp, "head": peer_head},
            device_id_type=MESH,
        )

    plane = dps * heads_axis
    over(plane, lambda step: plane_copy(step, place).start())

    each_wait_recv(a_copy, heads)
    assemble(heads - 1)

    over(plane, lambda step: plane_copy(step, lax.rem(place + step, plane)).wait_recv())
    everything = jnp.sum(plane_sums[...], axis=0)
    everything = jnp.sum(everything, axis=1, keepdims=True)
    everything = jnp.sum(everything, axis=0, keepdims=True)
    rms_ref[0] = jnp.sqrt(everything * (1.0 / total))[0, 0]

    def finish(head, carry):
        each_wait_send(own_copy, head)
        each_wait_send(a_copy, head)
        each_wait_send(b_copy, head)
        return carry

    lax.fori_loop(0, heads, finish, 0)
    each_wait_send(a_copy, heads)
    over(line, lambda step: line_copy(step).wait_send())
    over(plane, lambda step: plane_copy(step, place).wait_send())


def solution(mesh):
    line, dps, heads_axis = mesh.shape["seq"], mesh.shape["dp"], mesh.shape["head"]

    def shards(queries, key_rows, value_rows, out_grad, tile_image):
        _, rows, features = queries.shape
        heads = features // HEAD_DIM
        total = 3.0 * rows * features * line * dps * heads_axis
        result = jax.ShapeDtypeStruct((1, rows, features), jnp.bfloat16)
        tile = (4, TILE, HEAD_DIM)
        bf16, f32 = jnp.bfloat16, jnp.float32
        dma = pltpu.SemaphoreType.DMA
        vmem = pl.BlockSpec(memory_space=pltpu.VMEM)
        smem = pl.BlockSpec(memory_space=pltpu.SMEM)
        hbm = pl.BlockSpec(memory_space=pl.ANY)
        outputs = pl.pallas_call(
            functools.partial(
                kernel, heads=heads, line=line, dps=dps, heads_axis=heads_axis, total=total
            ),
            out_shape=(result, result, result, result, jax.ShapeDtypeStruct((1,), f32)),
            in_specs=[smem, hbm, hbm, hbm, hbm],
            out_specs=(vmem, vmem, vmem, vmem, smem),
            scratch_shapes=[
                pltpu.VMEM((heads, 4, ROWS, HEAD_DIM), bf16),
                pltpu.VMEM((heads, 4, ROWS, HEAD_DIM), bf16),
                pltpu.VMEM((2, heads + 1) + tile, bf16),
                pltpu.VMEM((2, heads + 1) + tile, bf16),
                pltpu.VMEM((2, heads) + tile, bf16),
                pltpu.VMEM((WINDOW, ROWS), f32),
                pltpu.VMEM((HEAD_DIM, ROWS), f32),
                pltpu.VMEM((HEAD_DIM, ROWS), f32),
                pltpu.VMEM((8, 128), f32),
                pltpu.VMEM((line, 8, 128), f32),
                pltpu.VMEM((dps * heads_axis, 8, 128), f32),
                dma((heads, 4)),
                dma((2, heads)),
                dma((2, heads)),
                dma((2, heads + 1)),
                dma((2, heads + 1)),
                dma((2, heads)),
                dma((2, heads)),
                dma((line,)),
                dma((line,)),
                dma((dps * heads_axis,)),
                dma((dps * heads_axis,)),
            ],
            compiler_params=pltpu.CompilerParams(
                collective_id=0, has_side_effects=True, vmem_limit_bytes=48 * 1024 * 1024
            ),
        )(tile_image, queries, key_rows, value_rows, out_grad)
        return outputs[:4] + (outputs[4].reshape(()),)

    wide = P("dp", "seq", "head")
    return jax.shard_map(
        shards,
        mesh=mesh,
        in_specs=(wide, wide, wide, wide, P("dp", None)),
        out_specs=(wide, wide, wide, wide, P()),
        check_vma=False,
    )
```

```python
import functools

import jax
import jax.numpy as jnp
from jax import lax
from jax.experimental import pallas as pl
from jax.experimental.pallas import tpu as pltpu
from jax.sharding import PartitionSpec as P

HEAD_DIM = 128
TILE = 128
OWN = 2
WINDOW = 8
ROWS = WINDOW * TILE
BLOCK = 256
LAG = 3
MESH = pl.DeviceIdType.MESH


def rows_of(tile, count=1):
    return pl.ds(tile * TILE, count * TILE)


def kernel(
    tiles_ref,
    q_hbm,
    k_hbm,
    v_hbm,
    g_hbm,
    o_ref,
    dq_ref,
    dk_ref,
    dv_ref,
    rms_ref,
    win,
    outs,
    stage,
    got_m,
    got_t,
    bias,
    dk_acc,
    dv_acc,
    squares,
    own_sum,
    line_sums,
    plane_sums,
    load_sem,
    m_send,
    m_recv,
    t_send,
    t_recv,
    token,
    line_send,
    line_recv,
    plane_send,
    plane_recv,
    *,
    heads,
    line,
    dps,
    heads_axis,
    total,
):
    me = lax.axis_index("seq")
    my_dp = lax.axis_index("dp")
    my_head = lax.axis_index("head")
    scale = HEAD_DIM ** (-0.5)
    has_left = me > 0
    has_right = me < line - 1
    left = jnp.maximum(me - 1, 0)
    right = jnp.minimum(me + 1, line - 1)
    tile_count = OWN * line

    def load(source, slot, head):
        return pltpu.make_async_copy(
            source.at[0, :, pl.ds(head * HEAD_DIM, HEAD_DIM)],
            win.at[head, slot, rows_of(3, 2), :],
            load_sem.at[head, slot],
        )

    def sent(source, target, send, recv, way):
        return pltpu.make_async_remote_copy(
            src_ref=source,
            dst_ref=target,
            send_sem=send,
            recv_sem=recv,
            device_id={"seq": right if way == 0 else left},
            device_id_type=MESH,
        )

    def m_copy(turn, way, source):
        return sent(
            source, got_m.at[way, turn], m_send.at[way, turn], m_recv.at[way, turn], way
        )

    def m_inputs(turn, way):
        return m_copy(turn, way, win.at[turn, :, rows_of(3, 2), :])

    def m_either(turn, way):
        return m_copy(turn, way, stage.at[way, turn - LAG])

    def m_results(turn, way):
        return m_copy(turn, way, outs.at[turn - LAG, :, rows_of(5 if way == 0 else 1, 2), :])

    def t_copy(head, way):
        return sent(
            got_m.at[way, head, :, rows_of(1 if way == 0 else 0), :],
            got_t.at[way, head],
            t_send.at[way, head],
            t_recv.at[way, head],
            way,
        )

    inner = jnp.logical_and(has_left, has_right)

    def m_start(copy, turn):
        @pl.when(has_right)
        def _():
            copy(turn, 0).start()

        @pl.when(has_left)
        def _():
            copy(turn, 1).start()

    def m_wait_recv(turn):
        @pl.when(has_left)
        def _():
            m_copy(turn, 0, got_m.at[0, turn]).wait_recv()

        @pl.when(has_right)
        def _():
            m_copy(turn, 1, got_m.at[1, turn]).wait_recv()

    def m_wait_send(copy, turn):
        @pl.when(has_right)
        def _():
            copy(turn, 0).wait_send()

        @pl.when(has_left)
        def _():
            copy(turn, 1).wait_send()

    def t_start(head):
        @pl.when(inner)
        def _():
            t_copy(head, 0).start()
            t_copy(head, 1).start()

    def t_wait_recv(head):
        @pl.when(me > 1)
        def _():
            t_copy(head, 0).wait_recv()

        @pl.when(me < line - 2)
        def _():
            t_copy(head, 1).wait_recv()

    def t_wait_send(head):
        @pl.when(inner)
        def _():
            t_copy(head, 0).wait_send()
            t_copy(head, 1).wait_send()

    for head in range(heads):
        for slot, source in enumerate((q_hbm, k_hbm, v_hbm, g_hbm)):
            load(source, slot, head).start()

    barrier = pltpu.get_barrier_semaphore()

    near = []

    def ring(axis, place, count, stride):
        length = count // stride
        hop = place // stride
        if length == 2:
            near.append(({axis: lax.rem(place + stride, count)}, len(near)))
        elif length > 2:
            first = len(near)
            near.append(({axis: lax.rem(hop + 1, length) * stride + lax.rem(place, stride)}, first + 1))
            near.append(
                ({axis: lax.rem(hop + length - 1, length) * stride + lax.rem(place, stride)}, first)
            )

    ring("seq", me, line, 1)
    ring("head", my_head, heads_axis, 1)
    cores = 2 if dps % 2 == 0 else 1
    ring("dp", my_dp, dps, cores)
    if cores == 2:
        near.append(({"dp": my_dp + 1 - 2 * lax.rem(my_dp, 2)}, len(near)))

    def give_tokens():
        for peer, heard in near:
            pl.semaphore_signal(token.at[heard], inc=1, device_id=peer, device_id_type=MESH)

    def take_tokens():
        for index in range(len(near)):
            pl.semaphore_wait(token.at[index], 1)

    def plane_peer(step):
        place = lax.rem(my_dp * heads_axis + my_head + step, dps * heads_axis)
        return place // heads_axis, lax.rem(place, heads_axis)

    for peer, _ in near:
        pl.semaphore_signal(barrier, inc=1, device_id=peer, device_id_type=MESH)

    images = []
    for place in range(WINDOW):
        tile = OWN * me - 3 + place
        image = tiles_ref[0, jnp.clip(tile, 0, tile_count - 1)]
        image = jnp.where(tile < 0, -1, image)
        images.append(jnp.where(tile >= tile_count, -2, image))

    def border(tiles):
        crossing = tiles[2] == tiles[3]
        a2, a3 = tiles[1] == tiles[2], tiles[0] == tiles[2]
        b2, b3 = tiles[4] == tiles[3], tiles[5] == tiles[3]
        both = jnp.logical_and(crossing, jnp.logical_and(a3, b3))
        fewer_right = jnp.logical_or(
            jnp.logical_and(a3, jnp.logical_not(b3)), jnp.logical_and(a2, jnp.logical_not(b2))
        )
        at_left = jnp.logical_and(crossing, fewer_right)
        at_right = jnp.logical_not(jnp.logical_or(at_left, both))
        return both, at_left, at_right

    left_both, left_at_left, left_at_right = border(images[0:6])
    right_both, right_at_left, right_at_right = border(images[2:8])
    in_left = jnp.logical_and(has_left, jnp.logical_or(left_both, left_at_right))
    in_right = jnp.logical_and(has_right, jnp.logical_or(right_both, right_at_left))
    here = (left_both, in_left, in_left, True, True, in_right, in_right, right_both)
    names = []
    for place, present in enumerate(here):
        names.append(images[place] if present is True else jnp.where(present, images[place], -3 - place))
    for row in range(WINDOW):
        for column in range(WINDOW):
            level = jnp.where(names[row] == names[column], 0.0, -jnp.inf).astype(jnp.float32)
            bias[row : row + 1, column * TILE : (column + 1) * TILE] = jnp.full(
                (1, TILE), level, jnp.float32
            )
    from_left = [jnp.logical_and(images[w] == images[2], left_at_left) for w in (3, 4)]
    from_right = [jnp.logical_and(images[w] == images[5], right_at_right) for w in (3, 4)]
    mine = {}
    for w in (1, 2):
        mine[w] = jnp.logical_and(images[w] == images[3], left_at_right)
    for w in (5, 6):
        mine[w] = jnp.logical_and(images[w] == images[4], right_at_left)
    for index, w in enumerate((3, 4)):
        mine[w] = jnp.logical_not(jnp.logical_or(from_left[index], from_right[index]))
    squares[...] = jnp.zeros((8, 128), jnp.float32)

    pl.semaphore_wait(barrier, len(near))

    def loaded(head):
        for slot, source in enumerate((q_hbm, k_hbm, v_hbm, g_hbm)):
            load(source, slot, head).wait()

    for head in range(2):
        loaded(head)
        m_start(m_inputs, head)
    hops = max(line // 2, heads_axis // 2 + dps // (2 * cores) + cores - 1)
    for _ in range(max(hops - 1 - heads, 1)):
        give_tokens()
        take_tokens()

    def add_squares(value, flag):
        wide = value.astype(jnp.float32)
        wide = jnp.sum((wide * wide).reshape(TILE // 8, 8, HEAD_DIM), axis=0)
        squares[...] += jnp.where(flag, wide, 0.0)

    def compute(head):
        dk_acc[...] = jnp.zeros((HEAD_DIM, ROWS), jnp.float32)
        dv_acc[...] = jnp.zeros((HEAD_DIM, ROWS), jnp.float32)
        lanes = (((1,), (1,)), ((), ()))
        rows = (((0,), (0,)), ((), ()))
        wide = jnp.float32

        def block(index, carry):
            here = pl.ds(pl.multiple_of(index * BLOCK, BLOCK), BLOCK)
            query = win[head, 0, here, :]
            grad = win[head, 3, here, :]
            keys = win[head, 1]
            values = win[head, 2]
            scores = lax.dot_general(query, keys, lanes, preferred_element_type=wide) * scale
            pieces = []
            for half in range(BLOCK // TILE):
                row = bias[pl.ds(index * (BLOCK // TILE) + half, 1), :]
                pieces.append(scores[half * TILE : (half + 1) * TILE] + row)
            scores = jnp.concatenate(pieces, axis=0)
            raised = jnp.exp(scores - jnp.max(scores, axis=1, keepdims=True))
            weights = raised * (1.0 / jnp.sum(raised, axis=1, keepdims=True))
            weights = weights.astype(jnp.bfloat16)
            out = jnp.dot(weights, values, preferred_element_type=wide).astype(jnp.bfloat16)
            outs[head, 0, here, :] = out
            delta = jnp.sum(grad.astype(wide) * out.astype(wide), axis=1, keepdims=True)
            dweights = lax.dot_general(grad, values, lanes, preferred_element_type=wide)
            dscores = (weights.astype(wide) * (dweights - delta)).astype(jnp.bfloat16)
            dquery = jnp.dot(dscores, keys, preferred_element_type=wide) * scale
            outs[head, 1, here, :] = dquery.astype(jnp.bfloat16)
            dk_acc[...] += lax.dot_general(query, dscores, rows, preferred_element_type=wide)
            dv_acc[...] += lax.dot_general(grad, weights, rows, preferred_element_type=wide)
            return carry

        lax.fori_loop(0, ROWS // BLOCK, block, 0)
        for w in range(1, WINDOW - 1):
            dk = jnp.transpose(dk_acc[:, w * TILE : (w + 1) * TILE] * scale).astype(jnp.bfloat16)
            dv = jnp.transpose(dv_acc[:, w * TILE : (w + 1) * TILE]).astype(jnp.bfloat16)
            outs[head, 2, rows_of(w), :] = dk
            outs[head, 3, rows_of(w), :] = dv
            add_squares(outs[head, 1, rows_of(w), :], mine[w])
            add_squares(dk, mine[w])
            add_squares(dv, mine[w])

    out_refs = (o_ref, dq_ref, dk_ref, dv_ref)

    def assemble(head):
        column = pl.ds(pl.multiple_of(head * HEAD_DIM, HEAD_DIM), HEAD_DIM)
        for slot, out_ref in enumerate(out_refs):
            for index in range(OWN):
                value = outs[head, slot, rows_of(3 + index), :]
                other = got_m[0, head + LAG, slot, rows_of(index), :]
                value = jnp.where(from_left[index], other, value)
                other = got_m[1, head + LAG, slot, rows_of(index), :]
                value = jnp.where(from_right[index], other, value)
                out_ref[0, rows_of(index), column] = value

    def fill_stage(turn):
        for way, switch, back in ((0, right_at_left, 5), (1, left_at_right, 1)):
            for slot in range(4):
                stage[way, turn - LAG, slot] = jnp.where(
                    switch,
                    outs[turn - LAG, slot, rows_of(back, 2), :],
                    win[turn, slot, rows_of(3, 2), :],
                )

    def arrive(head):
        m_wait_recv(head)
        t_start(head)
        pair = jnp.zeros((OWN * TILE, HEAD_DIM), jnp.bfloat16)
        for slot in range(4):
            win[head, slot, rows_of(1, 2), :] = jnp.where(in_left, got_m[0, head, slot], pair)
            win[head, slot, rows_of(5, 2), :] = jnp.where(in_right, got_m[1, head, slot], pair)

    arrive(0)
    loaded(2)
    m_start(m_inputs, 2)

    def step(head, carry):
        @pl.when(head < heads - 2)
        def _():
            arrive(head + 1)

        give_tokens()
        t_wait_recv(head)
        blank = jnp.zeros((TILE, HEAD_DIM), jnp.bfloat16)
        for slot in range(4):
            win[head, slot, rows_of(0), :] = jnp.where(left_both, got_t[0, head, slot], blank)
            win[head, slot, rows_of(7), :] = jnp.where(right_both, got_t[1, head, slot], blank)
        compute(head)

        @pl.when(head == heads - 3)
        def _():
            arrive(heads - 1)

        @pl.when(head + LAG < heads)
        def _():
            loaded(head + LAG)
            fill_stage(head + LAG)
            m_start(m_either, head + LAG)

        @pl.when(jnp.logical_and(head + LAG >= heads, head < heads - 1))
        def _():
            m_start(m_results, head + LAG)

        take_tokens()

        @pl.when(jnp.logical_and(head >= 2, head < heads - 1))
        def _():
            assemble(head - 2)

        return carry

    lax.fori_loop(0, heads, step, 0)

    own_sum[...] = jnp.sum(squares[...], axis=0, keepdims=True)
    line_sums[pl.ds(me, 1)] = own_sum[...][None]

    def line_copy(step):
        return pltpu.make_async_remote_copy(
            src_ref=own_sum,
            dst_ref=line_sums.at[me],
            send_sem=line_send.at[step],
            recv_sem=line_recv.at[me],
            device_id={"seq": lax.rem(me + step, line)},
            device_id_type=MESH,
        )

    def line_arrival(step):
        peer = lax.rem(me + step, line)
        return pltpu.make_async_remote_copy(
            src_ref=own_sum,
            dst_ref=line_sums.at[peer],
            send_sem=line_send.at[step],
            recv_sem=line_recv.at[peer],
            device_id={"seq": peer},
            device_id_type=MESH,
        )

    def over(count, action):
        def body(step, carry):
            action(step)
            return carry

        lax.fori_loop(1, count, body, 0)

    over(line, lambda step: line_copy(step).start())

    m_start(m_results, heads - 1 + LAG)
    for head in range(heads - LAG, heads - 1):
        m_wait_recv(head + LAG)
        assemble(head)

    over(line, lambda step: line_arrival(step).wait_recv())
    place = my_dp * heads_axis + my_head
    line_total = jnp.sum(line_sums[...], axis=0)
    plane_sums[pl.ds(place, 1)] = line_total[None]

    def plane_copy(step, slot):
        peer_dp, peer_head = plane_peer(step)
        return pltpu.make_async_remote_copy(
            src_ref=plane_sums.at[place],
            dst_ref=plane_sums.at[slot],
            send_sem=plane_send.at[step],
            recv_sem=plane_recv.at[slot],
            device_id={"dp": peer_dp, "head": peer_head},
            device_id_type=MESH,
        )

    plane = dps * heads_axis
    over(plane, lambda step: plane_copy(step, place).start())

    m_wait_recv(heads - 1 + LAG)
    assemble(heads - 1)

    over(plane, lambda step: plane_copy(step, lax.rem(place + step, plane)).wait_recv())
    everything = jnp.sum(plane_sums[...], axis=0)
    everything = jnp.sum(everything, axis=1, keepdims=True)
    everything = jnp.sum(everything, axis=0, keepdims=True)
    rms_ref[0] = jnp.sqrt(everything * (1.0 / total))[0, 0]

    for turn in range(heads + LAG):
        m_wait_send(m_inputs if turn < LAG else m_either if turn < heads else m_results, turn)
    for head in range(heads):
        t_wait_send(head)
    over(line, lambda step: line_copy(step).wait_send())
    over(plane, lambda step: plane_copy(step, place).wait_send())


def flush(*refs):
    sources, targets, sems = refs[:4], refs[4:8], refs[8]
    copies = [
        pltpu.make_async_copy(sources[slot], targets[slot], sems.at[slot]) for slot in range(4)
    ]
    for copy in copies:
        copy.start()
    for copy in copies:
        copy.wait()


def solution(mesh):
    line, dps, heads_axis = mesh.shape["seq"], mesh.shape["dp"], mesh.shape["head"]

    def shards(queries, key_rows, value_rows, out_grad, tile_image):
        _, rows, features = queries.shape
        heads = features // HEAD_DIM
        total = 3.0 * rows * features * line * dps * heads_axis
        result = jax.ShapeDtypeStruct((1, rows, features), jnp.bfloat16)
        tile, pair = (4, TILE, HEAD_DIM), (4, OWN * TILE, HEAD_DIM)
        bf16, f32 = jnp.bfloat16, jnp.float32
        dma = pltpu.SemaphoreType.DMA
        vmem = pl.BlockSpec(memory_space=pltpu.VMEM)
        smem = pl.BlockSpec(memory_space=pltpu.SMEM)
        hbm = pl.BlockSpec(memory_space=pltpu.HBM)
        anywhere = pl.BlockSpec(memory_space=pl.ANY)
        outputs = pl.pallas_call(
            functools.partial(
                kernel, heads=heads, line=line, dps=dps, heads_axis=heads_axis, total=total
            ),
            out_shape=(result, result, result, result, jax.ShapeDtypeStruct((1,), f32)),
            in_specs=[smem, hbm, hbm, hbm, hbm],
            out_specs=(vmem, vmem, vmem, vmem, smem),
            scratch_shapes=[
                pltpu.VMEM((heads, 4, ROWS, HEAD_DIM), bf16),
                pltpu.VMEM((heads, 4, ROWS, HEAD_DIM), bf16),
                pltpu.VMEM((2, heads - LAG) + pair, bf16),
                pltpu.VMEM((2, heads + LAG) + pair, bf16),
                pltpu.VMEM((2, heads) + tile, bf16),
                pltpu.VMEM((WINDOW, ROWS), f32),
                pltpu.VMEM((HEAD_DIM, ROWS), f32),
                pltpu.VMEM((HEAD_DIM, ROWS), f32),
                pltpu.VMEM((8, 128), f32),
                pltpu.VMEM((1, 128), f32),
                pltpu.VMEM((line, 1, 128), f32),
                pltpu.VMEM((dps * heads_axis, 1, 128), f32),
                dma((heads, 4)),
                dma((2, heads + LAG)),
                dma((2, heads + LAG)),
                dma((2, heads)),
                dma((2, heads)),
                pltpu.SemaphoreType.REGULAR((7,)),
                dma((line,)),
                dma((line,)),
                dma((dps * heads_axis,)),
                dma((dps * heads_axis,)),
            ],
            compiler_params=pltpu.CompilerParams(
                collective_id=0, has_side_effects=True, vmem_limit_bytes=48 * 1024 * 1024
            ),
        )(*[pltpu.with_memory_space_constraint(x, pltpu.HBM) for x in (tile_image, queries, key_rows, value_rows, out_grad)])
        written = pl.pallas_call(
            flush,
            out_shape=(result, result, result, result),
            in_specs=[anywhere] * 4,
            out_specs=(hbm, hbm, hbm, hbm),
            scratch_shapes=[dma((4,))],
            compiler_params=pltpu.CompilerParams(vmem_limit_bytes=8 * 1024 * 1024),
        )(*outputs[:4])
        return tuple(written) + (outputs[4].reshape(()),)

    wide = P("dp", "seq", "head")
    return jax.shard_map(
        shards,
        mesh=mesh,
        in_specs=(wide, wide, wide, wide, P("dp", None)),
        out_specs=(wide, wide, wide, wide, P()),
        check_vma=False,
    )
```

```python
import functools

import jax
import jax.numpy as jnp
from jax import lax
from jax.experimental import pallas as pl
from jax.experimental.pallas import tpu as pltpu
from jax.sharding import PartitionSpec as P

HEAD_DIM = 128
TILE = 128
OWN = 2
SIGHT = 8
SLOTS = 6
ROWS = SLOTS * TILE
LOG2_E = 1.4426950408889634
BLOCK = 256
LAG = 3
MESH = pl.DeviceIdType.MESH


def rows_of(tile, count=1):
    return pl.ds(tile * TILE, count * TILE)


def kernel(
    tiles_ref,
    q_hbm,
    k_hbm,
    v_hbm,
    g_hbm,
    o_ref,
    dq_ref,
    dk_ref,
    dv_ref,
    rms_ref,
    win,
    outs,
    stage,
    got_m,
    got_t,
    bias,
    dk_acc,
    dv_acc,
    squares,
    own_sum,
    line_sums,
    plane_sums,
    load_sem,
    m_send,
    m_recv,
    t_send,
    t_recv,
    token,
    line_send,
    line_recv,
    plane_send,
    plane_recv,
    *,
    heads,
    line,
    dps,
    heads_axis,
    total,
):
    me = lax.axis_index("seq")
    my_dp = lax.axis_index("dp")
    my_head = lax.axis_index("head")
    scale = HEAD_DIM ** (-0.5)
    has_left = me > 0
    has_right = me < line - 1
    left = jnp.maximum(me - 1, 0)
    right = jnp.minimum(me + 1, line - 1)
    tile_count = OWN * line

    def load(source, slot, head):
        return pltpu.make_async_copy(
            source.at[0, :, pl.ds(head * HEAD_DIM, HEAD_DIM)],
            win.at[head, slot, rows_of(2, 2), :],
            load_sem.at[head, slot],
        )

    def sent(source, target, send, recv, way):
        return pltpu.make_async_remote_copy(
            src_ref=source,
            dst_ref=target,
            send_sem=send,
            recv_sem=recv,
            device_id={"seq": right if way == 0 else left},
            device_id_type=MESH,
        )

    def m_copy(turn, way, source):
        return sent(
            source, got_m.at[way, turn], m_send.at[way, turn], m_recv.at[way, turn], way
        )

    def m_inputs(turn, way):
        return m_copy(turn, way, win.at[turn, :, rows_of(2, 2), :])

    def m_either(turn, way):
        return m_copy(turn, way, stage.at[way, turn - LAG])

    def m_results(turn, way):
        return m_copy(turn, way, outs.at[turn - LAG, :, rows_of(4 if way == 0 else 0, 2), :])

    def t_copy(head, way):
        return sent(
            got_m.at[way, head, :, rows_of(1 if way == 0 else 0), :],
            got_t.at[way, head],
            t_send.at[way, head],
            t_recv.at[way, head],
            way,
        )

    inner = jnp.logical_and(has_left, has_right)

    def m_start(copy, turn):
        @pl.when(has_right)
        def _():
            copy(turn, 0).start()

        @pl.when(has_left)
        def _():
            copy(turn, 1).start()

    def m_wait_recv(turn):
        @pl.when(has_left)
        def _():
            m_copy(turn, 0, got_m.at[0, turn]).wait_recv()

        @pl.when(has_right)
        def _():
            m_copy(turn, 1, got_m.at[1, turn]).wait_recv()

    def m_wait_send(copy, turn):
        @pl.when(has_right)
        def _():
            copy(turn, 0).wait_send()

        @pl.when(has_left)
        def _():
            copy(turn, 1).wait_send()

    def t_start(head):
        @pl.when(inner)
        def _():
            t_copy(head, 0).start()
            t_copy(head, 1).start()

    def t_wait_recv(head):
        @pl.when(me > 1)
        def _():
            t_copy(head, 0).wait_recv()

        @pl.when(me < line - 2)
        def _():
            t_copy(head, 1).wait_recv()

    def t_wait_send(head):
        @pl.when(inner)
        def _():
            t_copy(head, 0).wait_send()
            t_copy(head, 1).wait_send()

    for head in range(heads):
        for slot, source in enumerate((q_hbm, k_hbm, v_hbm, g_hbm)):
            load(source, slot, head).start()

    barrier = pltpu.get_barrier_semaphore()

    near = []

    def ring(axis, place, count, stride):
        length = count // stride
        hop = place // stride
        if length == 2:
            near.append(({axis: lax.rem(place + stride, count)}, len(near)))
        elif length > 2:
            first = len(near)
            near.append(({axis: lax.rem(hop + 1, length) * stride + lax.rem(place, stride)}, first + 1))
            near.append(
                ({axis: lax.rem(hop + length - 1, length) * stride + lax.rem(place, stride)}, first)
            )

    ring("seq", me, line, 1)
    ring("head", my_head, heads_axis, 1)
    cores = 2 if dps % 2 == 0 else 1
    ring("dp", my_dp, dps, cores)
    if cores == 2:
        near.append(({"dp": my_dp + 1 - 2 * lax.rem(my_dp, 2)}, len(near)))

    def give_tokens():
        for peer, heard in near:
            pl.semaphore_signal(token.at[heard], inc=1, device_id=peer, device_id_type=MESH)

    def take_tokens():
        for index in range(len(near)):
            pl.semaphore_wait(token.at[index], 1)

    def plane_peer(step):
        place = lax.rem(my_dp * heads_axis + my_head + step, dps * heads_axis)
        return place // heads_axis, lax.rem(place, heads_axis)

    for peer, _ in near:
        pl.semaphore_signal(barrier, inc=1, device_id=peer, device_id_type=MESH)

    images = []
    for place in range(SIGHT):
        tile = OWN * me - 3 + place
        image = tiles_ref[0, jnp.clip(tile, 0, tile_count - 1)]
        image = jnp.where(tile < 0, -1, image)
        images.append(jnp.where(tile >= tile_count, -2, image))

    def border(tiles):
        crossing = tiles[2] == tiles[3]
        a2, a3 = tiles[1] == tiles[2], tiles[0] == tiles[2]
        b2, b3 = tiles[4] == tiles[3], tiles[5] == tiles[3]
        both = jnp.logical_and(crossing, jnp.logical_and(a3, b3))
        fewer_right = jnp.logical_or(
            jnp.logical_and(a3, jnp.logical_not(b3)), jnp.logical_and(a2, jnp.logical_not(b2))
        )
        at_left = jnp.logical_and(crossing, fewer_right)
        at_right = jnp.logical_not(jnp.logical_or(at_left, both))
        return both, at_left, at_right

    left_both, left_at_left, left_at_right = border(images[0:6])
    right_both, right_at_left, right_at_right = border(images[2:8])
    in_left = jnp.logical_and(has_left, jnp.logical_or(left_both, left_at_right))
    in_right = jnp.logical_and(has_right, jnp.logical_or(right_both, right_at_left))
    names = [
        jnp.where(right_both, images[7], jnp.where(in_left, images[1], -3)),
        jnp.where(in_left, images[2], -4),
        images[3],
        images[4],
        jnp.where(in_right, images[5], -5),
        jnp.where(left_both, images[0], jnp.where(in_right, images[6], -6)),
    ]
    for row in range(SLOTS):
        for column in range(SLOTS):
            level = jnp.where(names[row] == names[column], 0.0, -jnp.inf).astype(jnp.float32)
            bias[row : row + 1, column * TILE : (column + 1) * TILE] = jnp.full(
                (1, TILE), level, jnp.float32
            )
    from_left = [jnp.logical_and(images[w] == images[2], left_at_left) for w in (3, 4)]
    from_right = [jnp.logical_and(images[w] == images[5], right_at_right) for w in (3, 4)]
    mine = {}
    for w in (1, 2):
        mine[w] = jnp.logical_and(images[w] == images[3], left_at_right)
    for w in (5, 6):
        mine[w] = jnp.logical_and(images[w] == images[4], right_at_left)
    for index, w in enumerate((3, 4)):
        mine[w] = jnp.logical_not(jnp.logical_or(from_left[index], from_right[index]))
    squares[...] = jnp.zeros((8, 128), jnp.float32)

    pl.semaphore_wait(barrier, len(near))

    def loaded(head):
        for slot, source in enumerate((q_hbm, k_hbm, v_hbm, g_hbm)):
            load(source, slot, head).wait()

    for head in range(2):
        loaded(head)
        m_start(m_inputs, head)
    hops = max(line // 2, heads_axis // 2 + dps // (2 * cores) + cores - 1)
    for _ in range(max(hops - 1 - heads, 1)):
        give_tokens()
        take_tokens()

    def add_squares(value, flag):
        wide = value.astype(jnp.float32)
        wide = jnp.sum((wide * wide).reshape(TILE // 8, 8, HEAD_DIM), axis=0)
        squares[...] += jnp.where(flag, wide, 0.0)

    def compute(head):
        dk_acc[...] = jnp.zeros((HEAD_DIM, ROWS), jnp.float32)
        dv_acc[...] = jnp.zeros((HEAD_DIM, ROWS), jnp.float32)
        lanes = (((1,), (1,)), ((), ()))
        rows = (((0,), (0,)), ((), ()))
        wide = jnp.float32

        def block(index, carry):
            here = pl.ds(pl.multiple_of(index * BLOCK, BLOCK), BLOCK)
            query = win[head, 0, here, :]
            grad = win[head, 3, here, :]
            keys = win[head, 1]
            values = win[head, 2]
            scores = lax.dot_general(query, keys, lanes, preferred_element_type=wide)
            scores = scores * (scale * LOG2_E)
            pieces = []
            for half in range(BLOCK // TILE):
                row = bias[pl.ds(index * (BLOCK // TILE) + half, 1), :]
                pieces.append(scores[half * TILE : (half + 1) * TILE] + row)
            scores = jnp.concatenate(pieces, axis=0)
            raised = jnp.exp2(scores - jnp.max(scores, axis=1, keepdims=True))
            weights = raised * (1.0 / jnp.sum(raised, axis=1, keepdims=True))
            weights = weights.astype(jnp.bfloat16)
            out = jnp.dot(weights, values, preferred_element_type=wide).astype(jnp.bfloat16)
            outs[head, 0, here, :] = out
            delta = jnp.sum(grad.astype(wide) * out.astype(wide), axis=1, keepdims=True)
            dweights = lax.dot_general(grad, values, lanes, preferred_element_type=wide)
            dscores = (weights.astype(wide) * (dweights - delta)).astype(jnp.bfloat16)
            dquery = jnp.dot(dscores, keys, preferred_element_type=wide) * scale
            outs[head, 1, here, :] = dquery.astype(jnp.bfloat16)
            dk_acc[...] += lax.dot_general(query, dscores, rows, preferred_element_type=wide)
            dv_acc[...] += lax.dot_general(grad, weights, rows, preferred_element_type=wide)
            return carry

        lax.fori_loop(0, ROWS // BLOCK, block, 0)
        for w in range(1, SLOTS + 1):
            slot = w - 1
            dk = jnp.transpose(dk_acc[:, slot * TILE : (slot + 1) * TILE] * scale).astype(jnp.bfloat16)
            dv = jnp.transpose(dv_acc[:, slot * TILE : (slot + 1) * TILE]).astype(jnp.bfloat16)
            outs[head, 2, rows_of(slot), :] = dk
            outs[head, 3, rows_of(slot), :] = dv
            add_squares(outs[head, 1, rows_of(slot), :], mine[w])
            add_squares(dk, mine[w])
            add_squares(dv, mine[w])

    out_refs = (o_ref, dq_ref, dk_ref, dv_ref)

    def assemble(head):
        column = pl.ds(pl.multiple_of(head * HEAD_DIM, HEAD_DIM), HEAD_DIM)
        for slot, out_ref in enumerate(out_refs):
            for index in range(OWN):
                value = outs[head, slot, rows_of(2 + index), :]
                other = got_m[0, head + LAG, slot, rows_of(index), :]
                value = jnp.where(from_left[index], other, value)
                other = got_m[1, head + LAG, slot, rows_of(index), :]
                value = jnp.where(from_right[index], other, value)
                out_ref[0, rows_of(index), column] = value

    def fill_stage(turn):
        for way, switch, back in ((0, right_at_left, 4), (1, left_at_right, 0)):
            for slot in range(4):
                stage[way, turn - LAG, slot] = jnp.where(
                    switch,
                    outs[turn - LAG, slot, rows_of(back, 2), :],
                    win[turn, slot, rows_of(2, 2), :],
                )

    def arrive(head):
        m_wait_recv(head)
        t_start(head)
        pair = jnp.zeros((OWN * TILE, HEAD_DIM), jnp.bfloat16)
        for slot in range(4):
            win[head, slot, rows_of(0, 2), :] = jnp.where(in_left, got_m[0, head, slot], pair)
            win[head, slot, rows_of(4, 2), :] = jnp.where(in_right, got_m[1, head, slot], pair)

    arrive(0)
    loaded(2)
    m_start(m_inputs, 2)

    def step(head, carry):
        @pl.when(head < heads - 2)
        def _():
            arrive(head + 1)

        give_tokens()
        t_wait_recv(head)
        for slot in range(4):
            for switch, way, outer in ((right_both, 1, 0), (left_both, 0, SLOTS - 1)):
                win[head, slot, rows_of(outer), :] = jnp.where(
                    switch, got_t[way, head, slot], win[head, slot, rows_of(outer), :]
                )
        compute(head)

        @pl.when(head == heads - 3)
        def _():
            arrive(heads - 1)

        @pl.when(head + LAG < heads)
        def _():
            loaded(head + LAG)
            fill_stage(head + LAG)
            m_start(m_either, head + LAG)

        @pl.when(jnp.logical_and(head + LAG >= heads, head < heads - 2))
        def _():
            m_start(m_results, head + LAG)

        take_tokens()

        @pl.when(jnp.logical_and(head >= 2, head < heads - 1))
        def _():
            assemble(head - 2)

        return carry

    lax.fori_loop(0, heads, step, 0)

    own_sum[...] = jnp.sum(squares[...], axis=0, keepdims=True)
    line_sums[pl.ds(me, 1)] = own_sum[...][None]

    def line_copy(step):
        return pltpu.make_async_remote_copy(
            src_ref=own_sum,
            dst_ref=line_sums.at[me],
            send_sem=line_send.at[step],
            recv_sem=line_recv.at[me],
            device_id={"seq": lax.rem(me + step, line)},
            device_id_type=MESH,
        )

    def line_arrival(step):
        peer = lax.rem(me + step, line)
        return pltpu.make_async_remote_copy(
            src_ref=own_sum,
            dst_ref=line_sums.at[peer],
            send_sem=line_send.at[step],
            recv_sem=line_recv.at[peer],
            device_id={"seq": peer},
            device_id_type=MESH,
        )

    def over(count, action):
        def body(step, carry):
            action(step)
            return carry

        lax.fori_loop(1, count, body, 0)

    over(line, lambda step: line_copy(step).start())

    m_start(m_results, heads - 2 + LAG)
    m_start(m_results, heads - 1 + LAG)
    for head in range(heads - LAG, heads - 1):
        m_wait_recv(head + LAG)
        assemble(head)

    over(line, lambda step: line_arrival(step).wait_recv())
    place = my_dp * heads_axis + my_head
    line_total = jnp.sum(line_sums[...], axis=0)
    plane_sums[pl.ds(place, 1)] = line_total[None]

    def plane_copy(step, slot):
        peer_dp, peer_head = plane_peer(step)
        return pltpu.make_async_remote_copy(
            src_ref=plane_sums.at[place],
            dst_ref=plane_sums.at[slot],
            send_sem=plane_send.at[step],
            recv_sem=plane_recv.at[slot],
            device_id={"dp": peer_dp, "head": peer_head},
            device_id_type=MESH,
        )

    plane = dps * heads_axis
    over(plane, lambda step: plane_copy(step, place).start())

    m_wait_recv(heads - 1 + LAG)
    assemble(heads - 1)

    over(plane, lambda step: plane_copy(step, lax.rem(place + step, plane)).wait_recv())
    everything = jnp.sum(plane_sums[...], axis=0)
    everything = jnp.sum(everything, axis=1, keepdims=True)
    everything = jnp.sum(everything, axis=0, keepdims=True)
    rms_ref[0] = jnp.sqrt(everything * (1.0 / total))[0, 0]

    for turn in range(heads + LAG):
        m_wait_send(m_inputs if turn < LAG else m_either if turn < heads else m_results, turn)
    for head in range(heads):
        t_wait_send(head)
    over(line, lambda step: line_copy(step).wait_send())
    over(plane, lambda step: plane_copy(step, place).wait_send())


def flush(*refs):
    sources, targets, sems = refs[:4], refs[4:8], refs[8]
    copies = [
        pltpu.make_async_copy(sources[slot], targets[slot], sems.at[slot]) for slot in range(4)
    ]
    for copy in copies:
        copy.start()
    for copy in copies:
        copy.wait()


def solution(mesh):
    line, dps, heads_axis = mesh.shape["seq"], mesh.shape["dp"], mesh.shape["head"]

    def shards(queries, key_rows, value_rows, out_grad, tile_image):
        _, rows, features = queries.shape
        heads = features // HEAD_DIM
        total = 3.0 * rows * features * line * dps * heads_axis
        result = jax.ShapeDtypeStruct((1, rows, features), jnp.bfloat16)
        tile, pair = (4, TILE, HEAD_DIM), (4, OWN * TILE, HEAD_DIM)
        bf16, f32 = jnp.bfloat16, jnp.float32
        dma = pltpu.SemaphoreType.DMA
        vmem = pl.BlockSpec(memory_space=pltpu.VMEM)
        smem = pl.BlockSpec(memory_space=pltpu.SMEM)
        hbm = pl.BlockSpec(memory_space=pltpu.HBM)
        anywhere = pl.BlockSpec(memory_space=pl.ANY)
        outputs = pl.pallas_call(
            functools.partial(
                kernel, heads=heads, line=line, dps=dps, heads_axis=heads_axis, total=total
            ),
            out_shape=(result, result, result, result, jax.ShapeDtypeStruct((1,), f32)),
            in_specs=[smem, hbm, hbm, hbm, hbm],
            out_specs=(vmem, vmem, vmem, vmem, smem),
            scratch_shapes=[
                pltpu.VMEM((heads, 4, ROWS, HEAD_DIM), bf16),
                pltpu.VMEM((heads, 4, ROWS, HEAD_DIM), bf16),
                pltpu.VMEM((2, heads - LAG) + pair, bf16),
                pltpu.VMEM((2, heads + LAG) + pair, bf16),
                pltpu.VMEM((2, heads) + tile, bf16),
                pltpu.VMEM((SLOTS, ROWS), f32),
                pltpu.VMEM((HEAD_DIM, ROWS), f32),
                pltpu.VMEM((HEAD_DIM, ROWS), f32),
                pltpu.VMEM((8, 128), f32),
                pltpu.VMEM((1, 128), f32),
                pltpu.VMEM((line, 1, 128), f32),
                pltpu.VMEM((dps * heads_axis, 1, 128), f32),
                dma((heads, 4)),
                dma((2, heads + LAG)),
                dma((2, heads + LAG)),
                dma((2, heads)),
                dma((2, heads)),
                pltpu.SemaphoreType.REGULAR((7,)),
                dma((line,)),
                dma((line,)),
                dma((dps * heads_axis,)),
                dma((dps * heads_axis,)),
            ],
            compiler_params=pltpu.CompilerParams(
                collective_id=0, has_side_effects=True, vmem_limit_bytes=48 * 1024 * 1024
            ),
        )(*[pltpu.with_memory_space_constraint(x, pltpu.HBM) for x in (tile_image, queries, key_rows, value_rows, out_grad)])
        written = pl.pallas_call(
            flush,
            out_shape=(result, result, result, result),
            in_specs=[anywhere] * 4,
            out_specs=(hbm, hbm, hbm, hbm),
            scratch_shapes=[dma((4,))],
            compiler_params=pltpu.CompilerParams(vmem_limit_bytes=8 * 1024 * 1024),
        )(*outputs[:4])
        return tuple(written) + (outputs[4].reshape(()),)

    wide = P("dp", "seq", "head")
    return jax.shard_map(
        shards,
        mesh=mesh,
        in_specs=(wide, wide, wide, wide, P("dp", None)),
        out_specs=(wide, wide, wide, wide, P()),
        check_vma=False,
    )
```

```python
import functools

import jax
import jax.numpy as jnp
from jax import lax
from jax.experimental import pallas as pl
from jax.experimental.pallas import tpu as pltpu
from jax.sharding import PartitionSpec as P

HEAD_DIM = 128
TILE = 128
OWN = 2
SIGHT = 8
SLOTS = 6
ROWS = SLOTS * TILE
LOG2_E = 1.4426950408889634
BLOCK = 768
LAG = 3
MESH = pl.DeviceIdType.MESH


def rows_of(tile, count=1):
    return pl.ds(tile * TILE, count * TILE)


def kernel(
    tiles_ref,
    q_hbm,
    k_hbm,
    v_hbm,
    g_hbm,
    o_ref,
    dq_ref,
    dk_ref,
    dv_ref,
    rms_ref,
    win,
    outs,
    stage,
    got_m,
    got_t,
    bias,
    dk_acc,
    dv_acc,
    squares,
    own_sum,
    line_sums,
    plane_sums,
    load_sem,
    m_send,
    m_recv,
    t_send,
    t_recv,
    token,
    line_send,
    line_recv,
    plane_send,
    plane_recv,
    *,
    heads,
    line,
    dps,
    heads_axis,
    total,
):
    me = lax.axis_index("seq")
    my_dp = lax.axis_index("dp")
    my_head = lax.axis_index("head")
    scale = HEAD_DIM ** (-0.5)
    has_left = me > 0
    has_right = me < line - 1
    left = jnp.maximum(me - 1, 0)
    right = jnp.minimum(me + 1, line - 1)
    tile_count = OWN * line

    def load(source, slot, head):
        return pltpu.make_async_copy(
            source.at[0, :, pl.ds(head * HEAD_DIM, HEAD_DIM)],
            win.at[head, slot, rows_of(2, 2), :],
            load_sem.at[head, slot],
        )

    def sent(source, target, send, recv, way):
        return pltpu.make_async_remote_copy(
            src_ref=source,
            dst_ref=target,
            send_sem=send,
            recv_sem=recv,
            device_id={"seq": right if way == 0 else left},
            device_id_type=MESH,
        )

    def m_copy(turn, way, source):
        return sent(
            source, got_m.at[way, turn], m_send.at[way, turn], m_recv.at[way, turn], way
        )

    def m_inputs(turn, way):
        return m_copy(turn, way, win.at[turn, :, rows_of(2, 2), :])

    def m_either(turn, way):
        return m_copy(turn, way, stage.at[way, turn - LAG])

    def m_results(turn, way):
        return m_copy(turn, way, outs.at[turn - LAG, :, rows_of(4 if way == 0 else 0, 2), :])

    def t_copy(head, way):
        return sent(
            got_m.at[way, head, :, rows_of(1 if way == 0 else 0), :],
            got_t.at[way, head],
            t_send.at[way, head],
            t_recv.at[way, head],
            way,
        )

    inner = jnp.logical_and(has_left, has_right)

    def m_start(copy, turn):
        @pl.when(has_right)
        def _():
            copy(turn, 0).start()

        @pl.when(has_left)
        def _():
            copy(turn, 1).start()

    def m_wait_recv(turn):
        @pl.when(has_left)
        def _():
            m_copy(turn, 0, got_m.at[0, turn]).wait_recv()

        @pl.when(has_right)
        def _():
            m_copy(turn, 1, got_m.at[1, turn]).wait_recv()

    def m_wait_send(copy, turn):
        @pl.when(has_right)
        def _():
            copy(turn, 0).wait_send()

        @pl.when(has_left)
        def _():
            copy(turn, 1).wait_send()

    def t_start(head):
        @pl.when(inner)
        def _():
            t_copy(head, 0).start()
            t_copy(head, 1).start()

    def t_wait_recv(head):
        @pl.when(me > 1)
        def _():
            t_copy(head, 0).wait_recv()

        @pl.when(me < line - 2)
        def _():
            t_copy(head, 1).wait_recv()

    def t_wait_send(head):
        @pl.when(inner)
        def _():
            t_copy(head, 0).wait_send()
            t_copy(head, 1).wait_send()

    for head in range(heads):
        for slot, source in enumerate((q_hbm, k_hbm, v_hbm, g_hbm)):
            load(source, slot, head).start()

    barrier = pltpu.get_barrier_semaphore()

    near = []

    def ring(axis, place, count, stride):
        length = count // stride
        hop = place // stride
        if length == 2:
            near.append(({axis: lax.rem(place + stride, count)}, len(near)))
        elif length > 2:
            first = len(near)
            near.append(({axis: lax.rem(hop + 1, length) * stride + lax.rem(place, stride)}, first + 1))
            near.append(
                ({axis: lax.rem(hop + length - 1, length) * stride + lax.rem(place, stride)}, first)
            )

    ring("seq", me, line, 1)
    ring("head", my_head, heads_axis, 1)
    cores = 2 if dps % 2 == 0 else 1
    ring("dp", my_dp, dps, cores)
    if cores == 2:
        near.append(({"dp": my_dp + 1 - 2 * lax.rem(my_dp, 2)}, len(near)))

    def give_tokens():
        for peer, heard in near:
            pl.semaphore_signal(token.at[heard], inc=1, device_id=peer, device_id_type=MESH)

    def take_tokens():
        for index in range(len(near)):
            pl.semaphore_wait(token.at[index], 1)

    def plane_peer(step):
        place = lax.rem(my_dp * heads_axis + my_head + step, dps * heads_axis)
        return place // heads_axis, lax.rem(place, heads_axis)

    for peer, _ in near:
        pl.semaphore_signal(barrier, inc=1, device_id=peer, device_id_type=MESH)

    images = []
    for place in range(SIGHT):
        tile = OWN * me - 3 + place
        image = tiles_ref[0, jnp.clip(tile, 0, tile_count - 1)]
        image = jnp.where(tile < 0, -1, image)
        images.append(jnp.where(tile >= tile_count, -2, image))

    def border(tiles):
        crossing = tiles[2] == tiles[3]
        a2, a3 = tiles[1] == tiles[2], tiles[0] == tiles[2]
        b2, b3 = tiles[4] == tiles[3], tiles[5] == tiles[3]
        both = jnp.logical_and(crossing, jnp.logical_and(a3, b3))
        fewer_right = jnp.logical_or(
            jnp.logical_and(a3, jnp.logical_not(b3)), jnp.logical_and(a2, jnp.logical_not(b2))
        )
        at_left = jnp.logical_and(crossing, fewer_right)
        at_right = jnp.logical_not(jnp.logical_or(at_left, both))
        return both, at_left, at_right

    left_both, left_at_left, left_at_right = border(images[0:6])
    right_both, right_at_left, right_at_right = border(images[2:8])
    in_left = jnp.logical_and(has_left, jnp.logical_or(left_both, left_at_right))
    in_right = jnp.logical_and(has_right, jnp.logical_or(right_both, right_at_left))
    names = [
        jnp.where(right_both, images[7], jnp.where(in_left, images[1], -3)),
        jnp.where(in_left, images[2], -4),
        images[3],
        images[4],
        jnp.where(in_right, images[5], -5),
        jnp.where(left_both, images[0], jnp.where(in_right, images[6], -6)),
    ]
    for row in range(SLOTS):
        for column in range(SLOTS):
            level = jnp.where(names[row] == names[column], 0.0, -jnp.inf).astype(jnp.float32)
            bias[row : row + 1, column * TILE : (column + 1) * TILE] = jnp.full(
                (1, TILE), level, jnp.float32
            )
    from_left = [jnp.logical_and(images[w] == images[2], left_at_left) for w in (3, 4)]
    from_right = [jnp.logical_and(images[w] == images[5], right_at_right) for w in (3, 4)]
    mine = {}
    for w in (1, 2):
        mine[w] = jnp.logical_and(images[w] == images[3], left_at_right)
    for w in (5, 6):
        mine[w] = jnp.logical_and(images[w] == images[4], right_at_left)
    for index, w in enumerate((3, 4)):
        mine[w] = jnp.logical_not(jnp.logical_or(from_left[index], from_right[index]))
    squares[...] = jnp.zeros((8, 128), jnp.float32)

    pl.semaphore_wait(barrier, len(near))

    def loaded(head):
        for slot, source in enumerate((q_hbm, k_hbm, v_hbm, g_hbm)):
            load(source, slot, head).wait()

    for head in range(2):
        loaded(head)
        m_start(m_inputs, head)
    hops = max(line // 2, heads_axis // 2 + dps // (2 * cores) + cores - 1)
    for _ in range(max(hops - 1 - heads, 1)):
        give_tokens()
        take_tokens()

    def add_squares(value, flag):
        wide = value.astype(jnp.float32)
        wide = jnp.sum((wide * wide).reshape(TILE // 8, 8, HEAD_DIM), axis=0)
        squares[...] += jnp.where(flag, wide, 0.0)

    def compute(head):
        lanes = (((1,), (1,)), ((), ()))
        rows = (((0,), (0,)), ((), ()))
        wide = jnp.float32

        def block(index, carry):
            here = pl.ds(0, BLOCK)
            query = win[head, 0, here, :]
            grad = win[head, 3, here, :]
            keys = win[head, 1]
            values = win[head, 2]
            scores = lax.dot_general(query, keys, lanes, preferred_element_type=wide)
            scores = scores * (scale * LOG2_E)
            pieces = []
            for half in range(BLOCK // TILE):
                row = bias[pl.ds(index * (BLOCK // TILE) + half, 1), :]
                pieces.append(scores[half * TILE : (half + 1) * TILE] + row)
            scores = jnp.concatenate(pieces, axis=0)
            raised = jnp.exp2(scores - jnp.max(scores, axis=1, keepdims=True))
            weights = raised * (1.0 / jnp.sum(raised, axis=1, keepdims=True))
            weights = weights.astype(jnp.bfloat16)
            out = jnp.dot(weights, values, preferred_element_type=wide).astype(jnp.bfloat16)
            outs[head, 0, here, :] = out
            delta = jnp.sum(grad.astype(wide) * out.astype(wide), axis=1, keepdims=True)
            dweights = lax.dot_general(grad, values, lanes, preferred_element_type=wide)
            dscores = (weights.astype(wide) * (dweights - delta)).astype(jnp.bfloat16)
            dquery = jnp.dot(dscores, keys, preferred_element_type=wide) * scale
            outs[head, 1, here, :] = dquery.astype(jnp.bfloat16)
            dk_acc[...] = lax.dot_general(query, dscores, rows, preferred_element_type=wide)
            dv_acc[...] = lax.dot_general(grad, weights, rows, preferred_element_type=wide)
            return carry

        block(0, 0)
        for w in range(1, SLOTS + 1):
            slot = w - 1
            dk = jnp.transpose(dk_acc[:, slot * TILE : (slot + 1) * TILE] * scale).astype(jnp.bfloat16)
            dv = jnp.transpose(dv_acc[:, slot * TILE : (slot + 1) * TILE]).astype(jnp.bfloat16)
            outs[head, 2, rows_of(slot), :] = dk
            outs[head, 3, rows_of(slot), :] = dv
            add_squares(outs[head, 1, rows_of(slot), :], mine[w])
            add_squares(dk, mine[w])
            add_squares(dv, mine[w])

    out_refs = (o_ref, dq_ref, dk_ref, dv_ref)

    def assemble(head):
        column = pl.ds(pl.multiple_of(head * HEAD_DIM, HEAD_DIM), HEAD_DIM)
        for slot, out_ref in enumerate(out_refs):
            for index in range(OWN):
                value = outs[head, slot, rows_of(2 + index), :]
                other = got_m[0, head + LAG, slot, rows_of(index), :]
                value = jnp.where(from_left[index], other, value)
                other = got_m[1, head + LAG, slot, rows_of(index), :]
                value = jnp.where(from_right[index], other, value)
                out_ref[0, rows_of(index), column] = value

    def fill_stage(turn):
        for way, switch, back in ((0, right_at_left, 4), (1, left_at_right, 0)):
            for slot in range(4):
                stage[way, turn - LAG, slot] = jnp.where(
                    switch,
                    outs[turn - LAG, slot, rows_of(back, 2), :],
                    win[turn, slot, rows_of(2, 2), :],
                )

    def arrive(head):
        m_wait_recv(head)
        t_start(head)
        pair = jnp.zeros((OWN * TILE, HEAD_DIM), jnp.bfloat16)
        for slot in range(4):
            win[head, slot, rows_of(0, 2), :] = jnp.where(in_left, got_m[0, head, slot], pair)
            win[head, slot, rows_of(4, 2), :] = jnp.where(in_right, got_m[1, head, slot], pair)

    arrive(0)
    loaded(2)
    m_start(m_inputs, 2)

    def step(head, carry):
        @pl.when(head < heads - 2)
        def _():
            arrive(head + 1)

        give_tokens()
        t_wait_recv(head)
        for slot in range(4):
            for switch, way, outer in ((right_both, 1, 0), (left_both, 0, SLOTS - 1)):
                win[head, slot, rows_of(outer), :] = jnp.where(
                    switch, got_t[way, head, slot], win[head, slot, rows_of(outer), :]
                )
        compute(head)

        @pl.when(head == heads - 3)
        def _():
            arrive(heads - 1)

        @pl.when(head + LAG < heads)
        def _():
            loaded(head + LAG)
            fill_stage(head + LAG)
            m_start(m_either, head + LAG)

        @pl.when(jnp.logical_and(head + LAG >= heads, head < heads - 2))
        def _():
            m_start(m_results, head + LAG)

        take_tokens()

        @pl.when(jnp.logical_and(head >= 2, head < heads - 1))
        def _():
            assemble(head - 2)

        return carry

    lax.fori_loop(0, heads, step, 0)

    own_sum[...] = jnp.sum(squares[...], axis=0, keepdims=True)
    line_sums[pl.ds(me, 1)] = own_sum[...][None]

    def line_copy(step):
        return pltpu.make_async_remote_copy(
            src_ref=own_sum,
            dst_ref=line_sums.at[me],
            send_sem=line_send.at[step],
            recv_sem=line_recv.at[me],
            device_id={"seq": lax.rem(me + step, line)},
            device_id_type=MESH,
        )

    def line_arrival(step):
        peer = lax.rem(me + step, line)
        return pltpu.make_async_remote_copy(
            src_ref=own_sum,
            dst_ref=line_sums.at[peer],
            send_sem=line_send.at[step],
            recv_sem=line_recv.at[peer],
            device_id={"seq": peer},
            device_id_type=MESH,
        )

    def over(count, action):
        for step in range(1, count):
            action(step)

    over(line, lambda step: line_copy(step).start())

    m_start(m_results, heads - 2 + LAG)
    m_start(m_results, heads - 1 + LAG)
    for head in range(heads - LAG, heads - 1):
        m_wait_recv(head + LAG)
        assemble(head)

    over(line, lambda step: line_arrival(step).wait_recv())
    place = my_dp * heads_axis + my_head
    line_total = jnp.sum(line_sums[...], axis=0)
    plane_sums[pl.ds(place, 1)] = line_total[None]

    def plane_copy(step, slot):
        peer_dp, peer_head = plane_peer(step)
        return pltpu.make_async_remote_copy(
            src_ref=plane_sums.at[place],
            dst_ref=plane_sums.at[slot],
            send_sem=plane_send.at[step],
            recv_sem=plane_recv.at[slot],
            device_id={"dp": peer_dp, "head": peer_head},
            device_id_type=MESH,
        )

    plane = dps * heads_axis
    over(plane, lambda step: plane_copy(step, place).start())

    m_wait_recv(heads - 1 + LAG)
    assemble(heads - 1)

    over(plane, lambda step: plane_copy(step, lax.rem(place + step, plane)).wait_recv())
    everything = jnp.sum(plane_sums[...], axis=0)
    everything = jnp.sum(everything, axis=1, keepdims=True)
    everything = jnp.sum(everything, axis=0, keepdims=True)
    rms_ref[0] = jnp.sqrt(everything * (1.0 / total))[0, 0]

    for turn in range(heads + LAG):
        m_wait_send(m_inputs if turn < LAG else m_either if turn < heads else m_results, turn)
    for head in range(heads):
        t_wait_send(head)
    over(line, lambda step: line_copy(step).wait_send())
    over(plane, lambda step: plane_copy(step, place).wait_send())


def flush(*refs):
    sources, targets, sems = refs[:4], refs[4:8], refs[8]
    copies = [
        pltpu.make_async_copy(sources[slot], targets[slot], sems.at[slot]) for slot in range(4)
    ]
    for copy in copies:
        copy.start()
    for copy in copies:
        copy.wait()


def solution(mesh):
    line, dps, heads_axis = mesh.shape["seq"], mesh.shape["dp"], mesh.shape["head"]

    def shards(queries, key_rows, value_rows, out_grad, tile_image):
        _, rows, features = queries.shape
        heads = features // HEAD_DIM
        total = 3.0 * rows * features * line * dps * heads_axis
        result = jax.ShapeDtypeStruct((1, rows, features), jnp.bfloat16)
        tile, pair = (4, TILE, HEAD_DIM), (4, OWN * TILE, HEAD_DIM)
        bf16, f32 = jnp.bfloat16, jnp.float32
        dma = pltpu.SemaphoreType.DMA
        vmem = pl.BlockSpec(memory_space=pltpu.VMEM)
        smem = pl.BlockSpec(memory_space=pltpu.SMEM)
        hbm = pl.BlockSpec(memory_space=pltpu.HBM)
        anywhere = pl.BlockSpec(memory_space=pl.ANY)
        outputs = pl.pallas_call(
            functools.partial(
                kernel, heads=heads, line=line, dps=dps, heads_axis=heads_axis, total=total
            ),
            out_shape=(result, result, result, result, jax.ShapeDtypeStruct((1,), f32)),
            in_specs=[smem, hbm, hbm, hbm, hbm],
            out_specs=(vmem, vmem, vmem, vmem, smem),
            scratch_shapes=[
                pltpu.VMEM((heads, 4, ROWS, HEAD_DIM), bf16),
                pltpu.VMEM((heads, 4, ROWS, HEAD_DIM), bf16),
                pltpu.VMEM((2, heads - LAG) + pair, bf16),
                pltpu.VMEM((2, heads + LAG) + pair, bf16),
                pltpu.VMEM((2, heads) + tile, bf16),
                pltpu.VMEM((SLOTS, ROWS), f32),
                pltpu.VMEM((HEAD_DIM, ROWS), f32),
                pltpu.VMEM((HEAD_DIM, ROWS), f32),
                pltpu.VMEM((8, 128), f32),
                pltpu.VMEM((1, 128), f32),
                pltpu.VMEM((line, 1, 128), f32),
                pltpu.VMEM((dps * heads_axis, 1, 128), f32),
                dma((heads, 4)),
                dma((2, heads + LAG)),
                dma((2, heads + LAG)),
                dma((2, heads)),
                dma((2, heads)),
                pltpu.SemaphoreType.REGULAR((7,)),
                dma((line,)),
                dma((line,)),
                dma((dps * heads_axis,)),
                dma((dps * heads_axis,)),
            ],
            compiler_params=pltpu.CompilerParams(
                collective_id=0, has_side_effects=True, vmem_limit_bytes=48 * 1024 * 1024
            ),
        )(*[pltpu.with_memory_space_constraint(x, pltpu.HBM) for x in (tile_image, queries, key_rows, value_rows, out_grad)])
        written = pl.pallas_call(
            flush,
            out_shape=(result, result, result, result),
            in_specs=[anywhere] * 4,
            out_specs=(hbm, hbm, hbm, hbm),
            scratch_shapes=[dma((4,))],
            compiler_params=pltpu.CompilerParams(vmem_limit_bytes=8 * 1024 * 1024),
        )(*outputs[:4])
        return tuple(written) + (outputs[4].reshape(()),)

    wide = P("dp", "seq", "head")
    return jax.shard_map(
        shards,
        mesh=mesh,
        in_specs=(wide, wide, wide, wide, P("dp", None)),
        out_specs=(wide, wide, wide, wide, P()),
        check_vma=False,
    )
```

```python
import functools

import jax
import jax.numpy as jnp
from jax import lax
from jax.experimental import pallas as pl
from jax.experimental.pallas import tpu as pltpu
from jax.sharding import PartitionSpec as P

HEAD_DIM = 128
TILE = 128
OWN = 2
SIGHT = 8
SLOTS = 6
ROWS = SLOTS * TILE
LOG2_E = 1.4426950408889634
BLOCK = 768
LAG = 3
MESH = pl.DeviceIdType.MESH


def rows_of(tile, count=1):
    return pl.ds(tile * TILE, count * TILE)


def kernel(
    tiles_ref,
    q_hbm,
    k_hbm,
    v_hbm,
    g_hbm,
    o_ref,
    dq_ref,
    dk_ref,
    dv_ref,
    rms_ref,
    win,
    outs,
    stage,
    got_m,
    got_t,
    bias,
    dk_acc,
    dv_acc,
    squares,
    own_sum,
    line_sums,
    plane_sums,
    load_sem,
    m_send,
    m_recv,
    t_send,
    t_recv,
    token,
    line_send,
    line_recv,
    plane_send,
    plane_recv,
    *,
    heads,
    line,
    dps,
    heads_axis,
    total,
):
    me = lax.axis_index("seq")
    my_dp = lax.axis_index("dp")
    my_head = lax.axis_index("head")
    scale = HEAD_DIM ** (-0.5)
    has_left = me > 0
    has_right = me < line - 1
    left = jnp.maximum(me - 1, 0)
    right = jnp.minimum(me + 1, line - 1)
    tile_count = OWN * line

    def load(source, slot, head):
        return pltpu.make_async_copy(
            source.at[0, :, pl.ds(head * HEAD_DIM, HEAD_DIM)],
            win.at[head, slot, rows_of(2, 2), :],
            load_sem.at[head, slot],
        )

    def sent(source, target, send, recv, way):
        return pltpu.make_async_remote_copy(
            src_ref=source,
            dst_ref=target,
            send_sem=send,
            recv_sem=recv,
            device_id={"seq": right if way == 0 else left},
            device_id_type=MESH,
        )

    def m_copy(turn, way, source):
        return sent(
            source, got_m.at[way, turn], m_send.at[way, turn], m_recv.at[way, turn], way
        )

    def m_inputs(turn, way):
        return m_copy(turn, way, win.at[turn, :, rows_of(2, 2), :])

    def m_either(turn, way):
        return m_copy(turn, way, stage.at[way, turn - LAG])

    def m_results(turn, way):
        return m_copy(turn, way, outs.at[turn - LAG, :, rows_of(4 if way == 0 else 0, 2), :])

    def t_copy(head, way):
        return sent(
            got_m.at[way, head, :, rows_of(1 if way == 0 else 0), :],
            got_t.at[way, head],
            t_send.at[way, head],
            t_recv.at[way, head],
            way,
        )

    inner = jnp.logical_and(has_left, has_right)

    def m_start(copy, turn):
        @pl.when(has_right)
        def _():
            copy(turn, 0).start()

        @pl.when(has_left)
        def _():
            copy(turn, 1).start()

    def m_wait_recv(turn):
        @pl.when(has_left)
        def _():
            m_copy(turn, 0, got_m.at[0, turn]).wait_recv()

        @pl.when(has_right)
        def _():
            m_copy(turn, 1, got_m.at[1, turn]).wait_recv()

    def m_wait_send(copy, turn):
        @pl.when(has_right)
        def _():
            copy(turn, 0).wait_send()

        @pl.when(has_left)
        def _():
            copy(turn, 1).wait_send()

    def t_start(head):
        @pl.when(inner)
        def _():
            t_copy(head, 0).start()
            t_copy(head, 1).start()

    def t_wait_recv(head):
        @pl.when(me > 1)
        def _():
            t_copy(head, 0).wait_recv()

        @pl.when(me < line - 2)
        def _():
            t_copy(head, 1).wait_recv()

    def t_wait_send(head):
        @pl.when(inner)
        def _():
            t_copy(head, 0).wait_send()
            t_copy(head, 1).wait_send()

    for head in range(heads):
        for slot, source in enumerate((q_hbm, k_hbm, v_hbm, g_hbm)):
            load(source, slot, head).start()

    barrier = pltpu.get_barrier_semaphore()

    near = []

    def ring(axis, place, count, stride):
        length = count // stride
        hop = place // stride
        if length == 2:
            near.append(({axis: lax.rem(place + stride, count)}, len(near)))
        elif length > 2:
            first = len(near)
            near.append(({axis: lax.rem(hop + 1, length) * stride + lax.rem(place, stride)}, first + 1))
            near.append(
                ({axis: lax.rem(hop + length - 1, length) * stride + lax.rem(place, stride)}, first)
            )

    ring("seq", me, line, 1)
    ring("head", my_head, heads_axis, 1)
    cores = 2 if dps % 2 == 0 else 1
    ring("dp", my_dp, dps, cores)
    if cores == 2:
        near.append(({"dp": my_dp + 1 - 2 * lax.rem(my_dp, 2)}, len(near)))

    def give_tokens():
        for peer, heard in near:
            pl.semaphore_signal(token.at[heard], inc=1, device_id=peer, device_id_type=MESH)

    def take_tokens():
        for index in range(len(near)):
            pl.semaphore_wait(token.at[index], 1)

    def plane_peer(step):
        place = lax.rem(my_dp * heads_axis + my_head + step, dps * heads_axis)
        return place // heads_axis, lax.rem(place, heads_axis)

    for peer, _ in near:
        pl.semaphore_signal(barrier, inc=1, device_id=peer, device_id_type=MESH)

    images = []
    for place in range(SIGHT):
        tile = OWN * me - 3 + place
        image = tiles_ref[0, jnp.clip(tile, 0, tile_count - 1)]
        image = jnp.where(tile < 0, -1, image)
        images.append(jnp.where(tile >= tile_count, -2, image))

    def border(tiles):
        crossing = tiles[2] == tiles[3]
        a2, a3 = tiles[1] == tiles[2], tiles[0] == tiles[2]
        b2, b3 = tiles[4] == tiles[3], tiles[5] == tiles[3]
        both = jnp.logical_and(crossing, jnp.logical_and(a3, b3))
        fewer_right = jnp.logical_or(
            jnp.logical_and(a3, jnp.logical_not(b3)), jnp.logical_and(a2, jnp.logical_not(b2))
        )
        at_left = jnp.logical_and(crossing, fewer_right)
        at_right = jnp.logical_not(jnp.logical_or(at_left, both))
        return both, at_left, at_right

    left_both, left_at_left, left_at_right = border(images[0:6])
    right_both, right_at_left, right_at_right = border(images[2:8])
    in_left = jnp.logical_and(has_left, jnp.logical_or(left_both, left_at_right))
    in_right = jnp.logical_and(has_right, jnp.logical_or(right_both, right_at_left))
    names = [
        jnp.where(right_both, images[7], jnp.where(in_left, images[1], -3)),
        jnp.where(in_left, images[2], -4),
        images[3],
        images[4],
        jnp.where(in_right, images[5], -5),
        jnp.where(left_both, images[0], jnp.where(in_right, images[6], -6)),
    ]
    for row in range(SLOTS):
        for column in range(SLOTS):
            level = jnp.where(names[row] == names[column], 0.0, -jnp.inf).astype(jnp.float32)
            bias[row : row + 1, column * TILE : (column + 1) * TILE] = jnp.full(
                (1, TILE), level, jnp.float32
            )
    from_left = [jnp.logical_and(images[w] == images[2], left_at_left) for w in (3, 4)]
    from_right = [jnp.logical_and(images[w] == images[5], right_at_right) for w in (3, 4)]
    mine = {}
    for w in (1, 2):
        mine[w] = jnp.logical_and(images[w] == images[3], left_at_right)
    for w in (5, 6):
        mine[w] = jnp.logical_and(images[w] == images[4], right_at_left)
    for index, w in enumerate((3, 4)):
        mine[w] = jnp.logical_not(jnp.logical_or(from_left[index], from_right[index]))
    squares[...] = jnp.zeros((8, 128), jnp.float32)

    pl.semaphore_wait(barrier, len(near))

    def loaded(head):
        for slot, source in enumerate((q_hbm, k_hbm, v_hbm, g_hbm)):
            load(source, slot, head).wait()

    for head in range(2):
        loaded(head)
        m_start(m_inputs, head)
    hops = max(line // 2, heads_axis // 2 + dps // (2 * cores) + cores - 1)
    for _ in range(max(hops - 1 - heads, 1)):
        give_tokens()
        take_tokens()

    def add_squares(value, flag):
        wide = value.astype(jnp.float32)
        wide = jnp.sum((wide * wide).reshape(TILE // 8, 8, HEAD_DIM), axis=0)
        squares[...] += jnp.where(flag, wide, 0.0)

    def compute(head):
        lanes = (((1,), (1,)), ((), ()))
        rows = (((0,), (0,)), ((), ()))
        wide = jnp.float32

        def block(index, carry):
            here = pl.ds(0, BLOCK)
            query = win[head, 0, here, :]
            grad = win[head, 3, here, :]
            keys = win[head, 1]
            values = win[head, 2]
            scores = lax.dot_general(query, keys, lanes, preferred_element_type=wide)
            scores = scores * (scale * LOG2_E)
            pieces = []
            for half in range(BLOCK // TILE):
                row = bias[pl.ds(index * (BLOCK // TILE) + half, 1), :]
                pieces.append(scores[half * TILE : (half + 1) * TILE] + row)
            scores = jnp.concatenate(pieces, axis=0)
            raised = jnp.exp2(scores - jnp.max(scores, axis=1, keepdims=True))
            weights = raised * (1.0 / jnp.sum(raised, axis=1, keepdims=True))
            weights = weights.astype(jnp.bfloat16)
            out = jnp.dot(weights, values, preferred_element_type=wide).astype(jnp.bfloat16)
            outs[head, 0, here, :] = out
            delta = jnp.sum(grad.astype(wide) * out.astype(wide), axis=1, keepdims=True)
            dweights = lax.dot_general(grad, values, lanes, preferred_element_type=wide)
            dscores = (weights.astype(wide) * (dweights - delta)).astype(jnp.bfloat16)
            dquery = jnp.dot(dscores, keys, preferred_element_type=wide) * scale
            outs[head, 1, here, :] = dquery.astype(jnp.bfloat16)
            dk_acc[...] = lax.dot_general(query, dscores, rows, preferred_element_type=wide)
            dv_acc[...] = lax.dot_general(grad, weights, rows, preferred_element_type=wide)
            return carry

        block(0, 0)
        for w in range(1, SLOTS + 1):
            slot = w - 1
            dk = jnp.transpose(dk_acc[:, slot * TILE : (slot + 1) * TILE] * scale).astype(jnp.bfloat16)
            dv = jnp.transpose(dv_acc[:, slot * TILE : (slot + 1) * TILE]).astype(jnp.bfloat16)
            outs[head, 2, rows_of(slot), :] = dk
            outs[head, 3, rows_of(slot), :] = dv
            add_squares(outs[head, 1, rows_of(slot), :], mine[w])
            add_squares(dk, mine[w])
            add_squares(dv, mine[w])

    out_refs = (o_ref, dq_ref, dk_ref, dv_ref)

    def assemble(head):
        column = pl.ds(pl.multiple_of(head * HEAD_DIM, HEAD_DIM), HEAD_DIM)
        for slot, out_ref in enumerate(out_refs):
            for index in range(OWN):
                value = outs[head, slot, rows_of(2 + index), :]
                other = got_m[0, head + LAG, slot, rows_of(index), :]
                value = jnp.where(from_left[index], other, value)
                other = got_m[1, head + LAG, slot, rows_of(index), :]
                value = jnp.where(from_right[index], other, value)
                out_ref[0, rows_of(index), column] = value

    def fill_stage(turn):
        for way, switch, back in ((0, right_at_left, 4), (1, left_at_right, 0)):
            for slot in range(4):
                stage[way, turn - LAG, slot] = jnp.where(
                    switch,
                    outs[turn - LAG, slot, rows_of(back, 2), :],
                    win[turn, slot, rows_of(2, 2), :],
                )

    def arrive(head):
        m_wait_recv(head)
        t_start(head)
        pair = jnp.zeros((OWN * TILE, HEAD_DIM), jnp.bfloat16)
        for slot in range(4):
            win[head, slot, rows_of(0, 2), :] = jnp.where(in_left, got_m[0, head, slot], pair)
            win[head, slot, rows_of(4, 2), :] = jnp.where(in_right, got_m[1, head, slot], pair)

    arrive(0)
    loaded(2)
    m_start(m_inputs, 2)

    def step(head, carry):
        @pl.when(head < heads - 2)
        def _():
            arrive(head + 1)

        give_tokens()
        t_wait_recv(head)
        for slot in range(4):
            for switch, way, outer in ((right_both, 1, 0), (left_both, 0, SLOTS - 1)):
                win[head, slot, rows_of(outer), :] = jnp.where(
                    switch, got_t[way, head, slot], win[head, slot, rows_of(outer), :]
                )
        compute(head)

        @pl.when(head == heads - 3)
        def _():
            arrive(heads - 1)

        @pl.when(head + LAG < heads)
        def _():
            loaded(head + LAG)
            fill_stage(head + LAG)
            m_start(m_either, head + LAG)

        take_tokens()

        @pl.when(jnp.logical_and(head >= 2, head < heads - 1))
        def _():
            assemble(head - 2)

        return carry

    lax.fori_loop(0, heads, step, 0)

    own_sum[...] = jnp.sum(squares[...], axis=0, keepdims=True)
    line_sums[pl.ds(me, 1)] = own_sum[...][None]

    def line_copy(step):
        return pltpu.make_async_remote_copy(
            src_ref=own_sum,
            dst_ref=line_sums.at[me],
            send_sem=line_send.at[step],
            recv_sem=line_recv.at[me],
            device_id={"seq": lax.rem(me + step, line)},
            device_id_type=MESH,
        )

    def line_arrival(step):
        peer = lax.rem(me + step, line)
        return pltpu.make_async_remote_copy(
            src_ref=own_sum,
            dst_ref=line_sums.at[peer],
            send_sem=line_send.at[step],
            recv_sem=line_recv.at[peer],
            device_id={"seq": peer},
            device_id_type=MESH,
        )

    def over(count, action):
        for step in range(1, count):
            action(step)

    over(line, lambda step: line_copy(step).start())

    m_start(m_results, heads - 3 + LAG)
    m_start(m_results, heads - 2 + LAG)
    m_start(m_results, heads - 1 + LAG)
    for head in range(heads - LAG, heads - 1):
        m_wait_recv(head + LAG)
        assemble(head)

    over(line, lambda step: line_arrival(step).wait_recv())
    place = my_dp * heads_axis + my_head
    line_total = jnp.sum(line_sums[...], axis=0)
    plane_sums[pl.ds(place, 1)] = line_total[None]

    def plane_copy(step, slot):
        peer_dp, peer_head = plane_peer(step)
        return pltpu.make_async_remote_copy(
            src_ref=plane_sums.at[place],
            dst_ref=plane_sums.at[slot],
            send_sem=plane_send.at[step],
            recv_sem=plane_recv.at[slot],
            device_id={"dp": peer_dp, "head": peer_head},
            device_id_type=MESH,
        )

    plane = dps * heads_axis
    over(plane, lambda step: plane_copy(step, place).start())

    m_wait_recv(heads - 1 + LAG)
    assemble(heads - 1)

    over(plane, lambda step: plane_copy(step, lax.rem(place + step, plane)).wait_recv())
    everything = jnp.sum(plane_sums[...], axis=0)
    everything = jnp.sum(everything, axis=1, keepdims=True)
    everything = jnp.sum(everything, axis=0, keepdims=True)
    rms_ref[0] = jnp.sqrt(everything * (1.0 / total))[0, 0]

    for turn in range(heads + LAG):
        m_wait_send(m_inputs if turn < LAG else m_either if turn < heads else m_results, turn)
    for head in range(heads):
        t_wait_send(head)
    over(line, lambda step: line_copy(step).wait_send())
    over(plane, lambda step: plane_copy(step, place).wait_send())


def flush(*refs):
    sources, targets, sems = refs[:4], refs[4:8], refs[8]
    copies = [
        pltpu.make_async_copy(sources[slot], targets[slot], sems.at[slot]) for slot in range(4)
    ]
    for copy in copies:
        copy.start()
    for copy in copies:
        copy.wait()


def solution(mesh):
    line, dps, heads_axis = mesh.shape["seq"], mesh.shape["dp"], mesh.shape["head"]

    def shards(queries, key_rows, value_rows, out_grad, tile_image):
        _, rows, features = queries.shape
        heads = features // HEAD_DIM
        total = 3.0 * rows * features * line * dps * heads_axis
        result = jax.ShapeDtypeStruct((1, rows, features), jnp.bfloat16)
        tile, pair = (4, TILE, HEAD_DIM), (4, OWN * TILE, HEAD_DIM)
        bf16, f32 = jnp.bfloat16, jnp.float32
        dma = pltpu.SemaphoreType.DMA
        vmem = pl.BlockSpec(memory_space=pltpu.VMEM)
        smem = pl.BlockSpec(memory_space=pltpu.SMEM)
        hbm = pl.BlockSpec(memory_space=pltpu.HBM)
        anywhere = pl.BlockSpec(memory_space=pl.ANY)
        outputs = pl.pallas_call(
            functools.partial(
                kernel, heads=heads, line=line, dps=dps, heads_axis=heads_axis, total=total
            ),
            out_shape=(result, result, result, result, jax.ShapeDtypeStruct((1,), f32)),
            in_specs=[smem, hbm, hbm, hbm, hbm],
            out_specs=(vmem, vmem, vmem, vmem, smem),
            scratch_shapes=[
                pltpu.VMEM((heads, 4, ROWS, HEAD_DIM), bf16),
                pltpu.VMEM((heads, 4, ROWS, HEAD_DIM), bf16),
                pltpu.VMEM((2, heads - LAG) + pair, bf16),
                pltpu.VMEM((2, heads + LAG) + pair, bf16),
                pltpu.VMEM((2, heads) + tile, bf16),
                pltpu.VMEM((SLOTS, ROWS), f32),
                pltpu.VMEM((HEAD_DIM, ROWS), f32),
                pltpu.VMEM((HEAD_DIM, ROWS), f32),
                pltpu.VMEM((8, 128), f32),
                pltpu.VMEM((1, 128), f32),
                pltpu.VMEM((line, 1, 128), f32),
                pltpu.VMEM((dps * heads_axis, 1, 128), f32),
                dma((heads, 4)),
                dma((2, heads + LAG)),
                dma((2, heads + LAG)),
                dma((2, heads)),
                dma((2, heads)),
                pltpu.SemaphoreType.REGULAR((7,)),
                dma((line,)),
                dma((line,)),
                dma((dps * heads_axis,)),
                dma((dps * heads_axis,)),
            ],
            compiler_params=pltpu.CompilerParams(
                collective_id=0, has_side_effects=True, vmem_limit_bytes=48 * 1024 * 1024
            ),
        )(*[pltpu.with_memory_space_constraint(x, pltpu.HBM) for x in (tile_image, queries, key_rows, value_rows, out_grad)])
        written = pl.pallas_call(
            flush,
            out_shape=(result, result, result, result),
            in_specs=[anywhere] * 4,
            out_specs=(hbm, hbm, hbm, hbm),
            scratch_shapes=[dma((4,))],
            compiler_params=pltpu.CompilerParams(vmem_limit_bytes=8 * 1024 * 1024),
        )(*outputs[:4])
        return tuple(written) + (outputs[4].reshape(()),)

    wide = P("dp", "seq", "head")
    return jax.shard_map(
        shards,
        mesh=mesh,
        in_specs=(wide, wide, wide, wide, P("dp", None)),
        out_specs=(wide, wide, wide, wide, P()),
        check_vma=False,
    )
```
